32 devices in a mesh: ctg: 8 (over y, x, core), br: 4 (over z).
Axes of the slice: x: 2, y: 2, z: 4, core: 2. Of those that a mesh axis runs over, the one named last changes fastest.
Arguments:
- base_vm: float32 [10240], P(('ctg', 'br')), may hold values from 0.95 to 1.05
- base_va: float32 [10240], P(('ctg', 'br')), may hold values from -0.6 to 0.6
- delta_state: float32 [64, 2, 10240], P('ctg', None, 'br'), may hold values from -0.18 to 0.18
- multipliers: float32 [64, 2, 10240], P('ctg', None, 'br'), may hold values from -6 to 6
- net_inj: float32 [64, 2, 10240], P('ctg', None, 'br'), may hold values from -6 to 6
- ang_grad: float32 [64, 10240], P('ctg', 'br'), may hold values from -6 to 6
- from_bus: int32 [13312], P('br'), may hold values from 0 to 10239
- to_bus: int32 [13312], P('br'), may hold values from 0 to 10239
- status: int32 [64, 13312], P('ctg', 'br'), may hold values 0 or 1
- conduct: float32 [13312], P('br'), may hold values from 1 to 5
- suscept: float32 [13312], P('br'), may hold values from -15 to -5
- charging: float32 [13312], P('br'), may hold values from 0.1 to 0.6
- rating: float32 [13312], P('br'), may hold values from 1 to 3
- slack: float32 [64, 13312], P('ctg', 'br'), may hold values from 0.05 to 2
- zdual: float32 [64, 13312], P('ctg', 'br'), may hold values from 0.05 to 2
Outputs:
- mismatch: float32 [64, 2, 10240], P('ctg', None, 'br')
- dual_res: float32 [64, 10240], P('ctg', 'br')
- limit_res: float32 [64, 13312], P('ctg', 'br')
- ctg_norms: float32 [64, 4], P('ctg')
- total_norms: float32 [4], replicated
The draws below stay inside these ranges and needn't reach their ends.
All inputs are finite; a program needn't handle non-finite values. No bound on the sum of `status` on one device may be relied on, other than what follows from the above.
Results may differ from the reference program's by a relative error of at most 0.0003.
Values sent between devices are 32-bit elements; how exact they have to be, the bound alone decides.
A program may use at most 64 MiB of HBM per device.

```python
import math
import jax
import jax.numpy as jnp
from jax import lax

NB = 10240
NL = 13312
CTG = 64


def place_ends(drawn, rng, smallest, high):
    longest = drawn.shape.index(max(drawn.shape))
    spots = []
    for shift in (0, 1):
        where = [jax.random.randint(jax.random.fold_in(rng, axis), (), 0, length) for axis, length in enumerate(drawn.shape)]
        where[longest] = (where[longest] + shift) % drawn.shape[longest]
        spots.append(tuple(where))
    return drawn.at[spots[0]].set(smallest).at[spots[1]].set(high)


def shard_levels(key, extent, shards, low, top_value):
    def one(position, shards_of):
        draws = jax.random.uniform(jax.random.fold_in(jax.random.fold_in(key, 6), position), (shards_of,), jnp.float32, low / len(shards), top_value / len(shards))
        return jnp.repeat(jnp.exp(draws), extent[position] // shards_of).reshape((-1,) + (1,) * (len(extent) - position - 1))

    loudness = one(*shards[0])
    for cut in shards[1:]:
        loudness = loudness * one(*cut)
    return loudness


def gaussian(key, extent, width, limit, split=(), dtype=jnp.bfloat16):
    array = jax.random.normal(key, extent, jnp.float32) * width
    if len(split) > 0:
        array = shard_levels(key, extent, split, -0.22, 0.18) * array
    return jnp.clip(array, min=-limit, max=limit).astype(dtype)


def setup_inputs(seed: int = 0) -> dict:
    streams_of = jax.random.split(jax.random.key(seed), 16)
    base_vm = jnp.clip(0.95 + 0.099999964 * jax.random.uniform(streams_of[0], (NB,), jnp.float32) ** shard_levels(streams_of[0], (NB,), ((0, 32),), -0.2, 0.2), 0.95, 1.05)
    base_va = gaussian(streams_of[1], (NB,), 0.1, 0.6, ((0, 32),), jnp.float32)
    delta_state = gaussian(streams_of[2], (CTG, 2, NB), 0.03, 0.18, ((0, 8), (2, 4)), jnp.float32)
    multipliers = gaussian(streams_of[3], (CTG, 2, NB), 1.0, 6.0, ((0, 8), (2, 4)), jnp.float32)
    net_inj = gaussian(streams_of[4], (CTG, 2, NB), 1.0, 6.0, ((0, 8), (2, 4)), jnp.float32)
    ang_grad = gaussian(streams_of[5], (CTG, NB), 1.0, 6.0, ((0, 8), (1, 4)), jnp.float32)
    from_bus = place_ends(jax.random.randint(streams_of[6], (NL,), 0, NB), jax.random.fold_in(streams_of[6], 1), 0, NB - 1).astype(jnp.int32)
    to_bus = place_ends(jax.random.randint(streams_of[7], (NL,), 0, NB), jax.random.fold_in(streams_of[7], 1), 0, NB - 1).astype(jnp.int32)
    status = place_ends((jax.random.randint(streams_of[8], (CTG, NL), 0, 8) < 7).astype(jnp.int32), jax.random.fold_in(streams_of[8], 1), 0, 1)
    conduct = jnp.clip(1.0 + 4.0 * jax.random.uniform(streams_of[9], (NL,), jnp.float32) ** shard_levels(streams_of[9], (NL,), ((0, 4),), -0.2, 0.2), 1.0, 5.0)
    suscept = jnp.clip(-15.0 + 10.0 * jax.random.uniform(streams_of[10], (NL,), jnp.float32) ** shard_levels(streams_of[10], (NL,), ((0, 4),), -0.2, 0.2), -15.0, -5.0)
    charging = jnp.clip(0.1 + 0.5 * jax.random.uniform(streams_of[11], (NL,), jnp.float32) ** shard_levels(streams_of[11], (NL,), ((0, 4),), -0.2, 0.2), 0.1, 0.6)
    rating = jnp.clip(1.0 + 2.0 * jax.random.uniform(streams_of[12], (NL,), jnp.float32) ** shard_levels(streams_of[12], (NL,), ((0, 4),), -0.2, 0.2), 1.0, 3.0)
    slack = jnp.clip(jnp.exp(math.log(2.0) - 3.6888794 * jax.random.uniform(streams_of[13], (CTG, NL), jnp.float32) ** shard_levels(streams_of[13], (CTG, NL), ((0, 8), (1, 4)), -0.2, 0.2)), 0.05, 2.0)
    zdual = jnp.clip(jnp.exp(math.log(2.0) - 3.6888794 * jax.random.uniform(streams_of[14], (CTG, NL), jnp.float32) ** shard_levels(streams_of[14], (CTG, NL), ((0, 8), (1, 4)), -0.2, 0.2)), 0.05, 2.0)
    return dict(base_vm=base_vm, base_va=base_va, delta_state=delta_state, multipliers=multipliers, net_inj=net_inj, ang_grad=ang_grad, from_bus=from_bus, to_bus=to_bus, status=status, conduct=conduct, suscept=suscept, charging=charging, rating=rating, slack=slack, zdual=zdual)


def branch_flows(volt_mag, volt_ang, mult_p, mult_q, from_idx, to_idx, conduct, suscept, charging, in_service):
    volt_from = volt_mag[:, from_idx]
    volt_to = volt_mag[:, to_idx]
    angle_diff = volt_ang[:, from_idx] - volt_ang[:, to_idx]
    cos_diff = jnp.cos(angle_diff)
    sin_diff = jnp.sin(angle_diff)
    volt_prod = volt_from * volt_to
    p_from = conduct * volt_from * volt_from - volt_prod * (conduct * cos_diff + suscept * sin_diff)
    q_from = -(suscept + charging) * volt_from * volt_from - volt_prod * (conduct * sin_diff - suscept * cos_diff)
    p_to = conduct * volt_to * volt_to - volt_prod * (conduct * cos_diff - suscept * sin_diff)
    q_to = -(suscept + charging) * volt_to * volt_to + volt_prod * (conduct * sin_diff + suscept * cos_diff)
    flow_dual = volt_prod * (mult_p[:, from_idx] * (conduct * sin_diff - suscept * cos_diff) - mult_q[:, from_idx] * (conduct * cos_diff + suscept * sin_diff) + mult_p[:, to_idx] * (conduct * sin_diff + suscept * cos_diff) + mult_q[:, to_idx] * (conduct * cos_diff - suscept * sin_diff))
    at_from = jnp.stack([p_from, q_from, flow_dual], 1) * in_service[:, None, :]
    at_to = jnp.stack([p_to, q_to, -flow_dual], 1) * in_service[:, None, :]
    return (at_from, at_to)

def reference(base_vm, base_va, delta_state, multipliers, net_inj, ang_grad, from_bus, to_bus, status, conduct, suscept, charging, rating, slack, zdual):
    volt_mag = base_vm[None, :] + delta_state[:, 0]
    volt_ang = base_va[None, :] + delta_state[:, 1]
    in_service = status.astype(jnp.float32)
    at_from, at_to = branch_flows(volt_mag, volt_ang, multipliers[:, 0], multipliers[:, 1], from_bus, to_bus, conduct, suscept, charging, in_service)
    scenarios = delta_state.shape[0]
    buses = delta_state.shape[2]
    summed = jnp.zeros((scenarios, 3, buses), jnp.float32)
    summed = summed.at[:, :, from_bus].add(at_from).at[:, :, to_bus].add(at_to)
    mismatch = summed[:, :2] - net_inj
    dual_res = summed[:, 2] + ang_grad
    limit_res = in_service * (at_from[:, 0] * at_from[:, 0] + at_from[:, 1] * at_from[:, 1] + slack - rating * rating)
    complement = in_service * (zdual * slack - 0.01)
    squares = jnp.stack([lax.optimization_barrier(jnp.sum(mismatch * mismatch, axis=(1, 2))), lax.optimization_barrier(jnp.sum(dual_res * dual_res, axis=1)), lax.optimization_barrier(jnp.sum(limit_res * limit_res, axis=1)), lax.optimization_barrier(jnp.sum(complement * complement, axis=1))], 1)
    ctg_norms = jnp.sqrt(squares)
    total_norms = jnp.sqrt(lax.optimization_barrier(jnp.sum(squares, axis=0)) / scenarios)
    return (mismatch, dual_res, limit_res, ctg_norms, total_norms)
```

```python
import functools
import math

import jax
import jax.numpy as jnp
from jax import lax
from jax.experimental import pallas as pl
from jax.experimental.pallas import tpu as pltpu
from jax.sharding import PartitionSpec as P

LANES = 128
SPAN = 256
SUB = 8
PACK = 16
MESH = pl.DeviceIdType.MESH


def sin_cos(x):
    y = x * x
    sin_c = (1 / 6227020800, -1 / 39916800, 1 / 362880, -1 / 5040, 1 / 120, -1 / 6)
    cos_c = (-1 / 87178291200, 1 / 479001600, -1 / 3628800, 1 / 40320, -1 / 720, 1 / 24, -0.5)
    s = jnp.full_like(y, sin_c[0])
    for c in sin_c[1:]:
        s = s * y + c
    k = jnp.full_like(y, cos_c[0])
    for c in cos_c[1:]:
        k = k * y + c
    return x + x * y * s, 1.0 + y * k


def packing(per):
    width = 6 * per
    group = width * PACK // math.gcd(width, PACK)
    starts = [(SUB * h) % width for h in range(group // SUB)]
    return width, group, starts, max(starts) + SUB


def body(
    groups, ranks,
    bvm, bva, delta, mult, net_h, ang_h, frm, to, status_t, con, sus, cha, rat, status_h, slack_h, zdual_h,
    mis_out, dual_out, lim_out, norm_out, tot_out,
    bown, bslot, volts, table, ends, par, stat, picks, vals, acc, res, rbuf, flow, rflow,
    sqs, sqbuf, rowbuf, net, ang, status, slack, zdual, rate,
    local, send, recv, base_send, base_recv, sq_send, sq_recv,
):
    grp, me = lax.axis_index("ctg"), lax.axis_index("br")
    count = groups * ranks
    mine = grp * ranks + me
    scen, _, nb = delta.shape
    per = scen // ranks
    rows = frm.shape[0]
    total = rows * ranks
    pad = rflow.shape[0] // scen
    bf16 = jnp.bfloat16

    def cols_of(src):
        return pl.ds(pl.multiple_of(src * nb, LANES), nb)

    def rows_of(src):
        return pl.ds(src * rows, rows)

    def scen_of(src):
        return pl.ds(src * per, per)

    pairs = [(bvm, bown.at[0, 0]), (bva, bown.at[1, 0])]
    pairs += [(delta.at[:, q], volts.at[q]) for q in range(2)]
    pairs += [(frm, ends.at[0, rows_of(me)]), (to, ends.at[1, rows_of(me)])]
    pairs += [(p, par.at[i, rows_of(me)]) for i, p in enumerate((con, sus, cha))]
    early = len(pairs)
    pairs += [(delta.at[scen_of(me), q], table.at[pl.ds(q * per, per), cols_of(me)]) for q in range(2)]
    pairs += [(mult.at[scen_of(me), q], table.at[pl.ds((2 + q) * per, per), cols_of(me)]) for q in range(2)]
    pairs += [(status_t.at[:, me * per + s], stat.at[s, rows_of(me)]) for s in range(per)]
    middle = len(pairs)
    pairs += [(net_h.at[:, q], net.at[q]) for q in range(2)]
    pairs += [(ang_h, ang), (status_h, status), (slack_h, slack), (zdual_h, zdual), (rat, rate)]
    copies = [pltpu.make_async_copy(a, b, local.at[i]) for i, (a, b) in enumerate(pairs)]
    for copy in copies:
        copy.start()

    barrier = pltpu.get_barrier_semaphore()

    def greet(i, carry):
        peer = lax.rem(mine + i, count)
        pl.semaphore_signal(
            barrier, inc=1, device_id=(peer // ranks, lax.rem(peer, ranks)), device_id_type=MESH
        )
        return carry

    lax.fori_loop(1, count, greet, 0)
    acc[...] = jnp.zeros_like(acc)
    sqs[...] = jnp.zeros_like(sqs)
    for copy in copies[:early]:
        copy.wait()
    pl.semaphore_wait(barrier, count - 1)

    def toward(step):
        return lax.rem(me - step + ranks, ranks)

    def origin(step):
        return lax.rem(me + step, ranks)

    def remote(src, dst, kind, step):
        return pltpu.make_async_remote_copy(
            src_ref=src, dst_ref=dst, send_sem=send.at[kind, step], recv_sem=recv.at[kind, step],
            device_id=(grp, toward(step)), device_id_type=MESH,
        )

    def send_ends(step):
        return [remote(ends.at[:, rows_of(me)], ends.at[:, rows_of(me)], 0, step)]

    def send_mult(step):
        return [
            remote(mult.at[scen_of(toward(step)), q], table.at[pl.ds((2 + q) * per, per), cols_of(me)], 1 + q, step)
            for q in range(2)
        ]

    def send_volts(step):
        return [
            remote(volts.at[q, scen_of(toward(step))], table.at[pl.ds(q * per, per), cols_of(me)], 3 + q, step)
            for q in range(2)
        ]

    def send_par(step):
        return [remote(par.at[:, rows_of(me)], par.at[:, rows_of(me)], 5, step)] + [
            remote(status_t.at[:, toward(step) * per + s], stat.at[s, rows_of(me)], 6 + s, step)
            for s in range(per)
        ]

    def send_res(step):
        return [remote(res.at[toward(step)], rbuf.at[:, scen_of(me)], 6 + per, step)]

    def send_flow(step):
        return [
            remote(flow.at[s, rows_of(toward(step))], rflow.at[pl.ds((me * per + s) * pad, rows)], 7 + per + s, step)
            for s in range(per)
        ]

    def send_sq(step):
        return [remote(sqbuf.at[me], sqbuf.at[me], 7 + 2 * per, step)]

    for step in range(1, ranks):
        for copy in send_ends(step):
            copy.start()

    home = mine // groups

    def base_copy(i):
        return pltpu.make_async_remote_copy(
            src_ref=bown, dst_ref=bslot.at[mine - home * groups],
            send_sem=base_send.at[i], recv_sem=base_recv.at[mine - home * groups],
            device_id=(i, home), device_id_type=MESH,
        )

    def begin_base(i, c):
        @pl.when(jnp.logical_or(i != grp, home != me))
        def _():
            base_copy(i).start()
        return c

    lax.fori_loop(0, groups, begin_base, 0)

    @pl.when(home == me)
    def _():
        bslot[mine - me * groups] = bown[...]

    for step in range(1, ranks):
        for copy in send_mult(step):
            copy.start()

    def end_base(i, c):
        @pl.when(jnp.logical_or(i != grp, home != me))
        def _():
            base_copy(i).wait_send()

        @pl.when(me * groups + i != mine)
        def _():
            pltpu.make_async_remote_copy(
                src_ref=bown, dst_ref=bslot.at[i], send_sem=base_send.at[i], recv_sem=base_recv.at[i],
                device_id=(i, home), device_id_type=MESH,
            ).wait_recv()
        return c

    lax.fori_loop(0, groups, end_base, 0)
    for copy in copies[early:middle]:
        copy.wait()
    for q in range(2):
        base = jnp.concatenate([bslot[i, q] for i in range(groups)], axis=1)
        volts[q] = volts[q] + base
        table[q * per : (q + 1) * per, cols_of(me)] = table[q * per : (q + 1) * per, cols_of(me)] + base

    for step in range(1, ranks):
        for copy in send_volts(step):
            copy.start()
    for step in range(1, ranks):
        for copy in send_par(step):
            copy.start()

    tiles = nb // LANES

    def look(spot, src, found):
        low, tile = spot & (LANES - 1), (spot >> 7) - src * tiles
        for k in range(tiles):
            piece = jnp.take_along_axis(
                table[:, pl.ds(pl.multiple_of(src * nb + k * LANES, LANES), LANES)],
                low, axis=1, mode="promise_in_bounds",
            )
            found = jnp.where(tile == k, piece, found)
        return found

    def spot_of(end, r):
        return jnp.broadcast_to(ends[end, pl.ds(r, 1), :], (SUB, LANES))

    def slot_of(r):
        return pl.ds(pl.multiple_of(r * SUB, SUB), SUB)

    unroll = 2 if rows % 2 == 0 else 1
    early_steps = max(1, ranks // 2)

    def scan_rows(src, block, fresh):
        def some(t, c):
            for o in range(unroll):
                r = block * rows + t * unroll + o
                for end in range(2):
                    start = jnp.zeros((SUB, LANES), jnp.float32) if fresh else picks[end, slot_of(r), :]
                    picks[end, slot_of(r), :] = look(spot_of(end, r), src, start)
            return c

        lax.fori_loop(0, rows // unroll, some, 0)

    for block in range(ranks):
        if block > 0:
            for copy in send_ends(block):
                copy.wait()
        scan_rows(me, origin(block), True)
    for step in range(1, early_steps):
        for copy in send_mult(step) + send_volts(step):
            copy.wait()
        lax.fori_loop(0, ranks, lambda b, c, step=step: (scan_rows(origin(step), b, False), c)[1], 0)
    for step in range(early_steps, ranks):
        for copy in send_mult(step) + send_volts(step):
            copy.wait()

    for copy in copies[middle:]:
        copy.wait()

    chunks = total // SUB
    first = (me * rows + SUB - 1) // SUB
    ahead = first * SUB - me * rows

    def chunk_of(i):
        return lax.rem(first + i, chunks)

    def pick(i):
        at = chunk_of(i) * SUB
        for end in range(2):
            for t in range(SUB):
                r = at + t
                spot = spot_of(end, r)
                found = picks[end, slot_of(r), :]
                for step in range(early_steps, ranks):
                    found = look(spot, origin(step), found)
                picks[end, slot_of(r), :] = found

    width, group, starts, entries = packing(per)
    spans = table.shape[1] // SPAN
    tps = group // width
    parts = group // PACK
    iota16 = lax.broadcasted_iota(jnp.int32, (PACK, LANES), 0)
    label = lax.broadcasted_iota(jnp.int32, (SPAN, LANES), 0).astype(bf16)
    shift = [((iota16 + PACK * p) // width).astype(bf16) for p in range(parts)]

    def process(i):
        at = pl.multiple_of(chunk_of(i) * SUB, SUB)
        here = pl.ds(at, SUB)

        def quantity(end, q, s):
            return picks[end, pl.ds(at * SUB + q * per + s, SUB, stride=SUB), :]

        seen = [[[quantity(end, q, s) for s in range(per)] for q in range(4)] for end in range(2)]
        pick(jnp.minimum(i + 1, chunks - 1))
        g, b, h = par[0, here, :], par[1, here, :], par[2, here, :]
        bh = -(b + h)
        for s in range(per):
            live = stat[s, here, :].astype(jnp.float32)
            vf, vt = seen[0][0][s], seen[1][0][s]
            sn, cs = sin_cos(seen[0][1][s] - seen[1][1][s])
            u = vf * vt
            gc_bs, gc_mbs = g * cs + b * sn, g * cs - b * sn
            gs_bc, gs_mbc = g * sn + b * cs, g * sn - b * cs
            pf = live * (g * vf * vf - u * gc_bs)
            qf = live * (bh * vf * vf - u * gs_mbc)
            pt = live * (g * vt * vt - u * gc_mbs)
            qt = live * (bh * vt * vt + u * gs_bc)
            fd = live * u * (
                seen[0][2][s] * gs_mbc - seen[0][3][s] * gc_bs
                + seen[1][2][s] * gs_bc + seen[1][3][s] * gc_mbs
            )
            flow[s, here, :] = pf * pf + qf * qf
            for end, terms in ((0, (pf, qf, fd)), (1, (pt, qt, -fd))):
                for q, term in enumerate(terms):
                    head = term.astype(bf16).astype(jnp.float32)
                    tail = term - head
                    for v, x in ((q * per + s, head), ((3 + q) * per + s, tail)):
                        for e in range(v, entries, width):
                            vals[end, e * SUB : (e + 1) * SUB, :] = x
        sums = None
        for end in range(2):
            for pair in range(SUB // 2):
                lefts, hots = [], []
                for t in (2 * pair, 2 * pair + 1):
                    spot = jnp.broadcast_to(ends[end, pl.ds(at + t, 1), :], (PACK, LANES))
                    high = (spot >> 8).astype(bf16)
                    low = (spot & (SPAN - 1)).astype(bf16)
                    low = jnp.concatenate([low] * (SPAN // PACK), axis=0)
                    hots.append(jnp.where(low == label, bf16(1), bf16(0)))
                    half = {
                        s0: vals[end, pl.ds(s0 * SUB + t, SUB, stride=SUB), :] for s0 in set(starts)
                    }
                    tile = [
                        jnp.concatenate([half[starts[2 * p]], half[starts[2 * p + 1]]], axis=0).astype(bf16)
                        for p in range(parts)
                    ]
                    level = [high - shift[p] for p in range(parts)]
                    lefts.append(jnp.concatenate([
                        jnp.where(level[p] == bf16(j * tps), tile[p], bf16(0))
                        for j in range(spans // tps) for p in range(parts)
                    ], axis=0))
                term = lax.dot_general(
                    jnp.concatenate(lefts, axis=1), jnp.concatenate(hots, axis=1),
                    (((1,), (1,)), ((), ())), preferred_element_type=jnp.float32,
                )
                sums = term if sums is None else sums + term
        acc[...] += sums

    pick(0)

    def advance(i, c):
        done = ahead + i * SUB

        for step in range(1, ranks):
            @pl.when(jnp.logical_and(done + SUB > step * rows, jnp.logical_or(done <= step * rows, i == 0)))
            def _(step=step):
                for copy in send_par(step):
                    copy.wait()

        process(i)

        for step in range(1, ranks):
            @pl.when(jnp.logical_and(done + SUB >= (step + 1) * rows, done < (step + 1) * rows))
            def _(step=step):
                for copy in send_flow(ranks - step):
                    copy.start()
        return c

    lax.fori_loop(0, chunks, advance, 0)

    quarter = nb // SPAN
    for dest in range(ranks):
        for k in range(dest * quarter, (dest + 1) * quarter):
            row = (k // tps) * group + (k % tps) * width
            both = acc[row : row + 3 * per, :] + acc[row + 3 * per : row + width, :]
            for q in range(3):
                at = (k - dest * quarter) * SPAN
                res[dest, q, :, at : at + SPAN] = both[q * per : (q + 1) * per, :]

        @pl.when(dest == me)
        def _(dest=dest):
            for q in range(3):
                rbuf[q, dest * per : (dest + 1) * per, :] = res[dest, q]

        for step in range(1, ranks):
            @pl.when(dest == toward(step))
            def _(step=step):
                for copy in send_res(step):
                    copy.start()

    for dest in range(ranks):
        @pl.when(dest == me)
        def _(dest=dest):
            for s in range(per):
                at = (dest * per + s) * pad
                rflow[at : at + rows, :] = flow[s, dest * rows : (dest + 1) * rows, :]

    live_own = status[...].astype(jnp.float32)
    comp = live_own * (zdual[...] * slack[...] - 0.01)
    sqs[:, 3:4] = jnp.sum(comp * comp, axis=1, keepdims=True)
    for step in range(1, ranks):
        for copy in send_flow(step):
            copy.wait()
    power = jnp.zeros((scen, LANES), jnp.float32)
    for r in range(rows):
        at = slice(r * LANES, (r + 1) * LANES)
        limit = rate[r : r + 1, :]
        lim = status[:, at].astype(jnp.float32) * (
            rflow[pl.ds(r, scen, stride=pad), :] + slack[:, at] - limit * limit
        )
        lim_out[:, at] = lim
        power = power + lim * lim
    sqs[:, 2:3] = jnp.sum(power, axis=1, keepdims=True)

    for step in range(1, ranks):
        for copy in send_res(step):
            copy.wait()
    power = None
    for q in range(2):
        row = rbuf[q] - net[q]
        mis_out[q] = row
        power = row * row if power is None else power + row * row
    sqs[:, 0:1] = jnp.sum(power, axis=1, keepdims=True)
    dual = rbuf[2] + ang[...]
    dual_out[...] = dual
    sqs[:, 1:2] = jnp.sum(dual * dual, axis=1, keepdims=True)

    sqbuf[me] = sqs[...]
    rowbuf[mine] = jnp.sum(sqs[...], axis=0, keepdims=True)
    for step in range(1, ranks):
        for copy in send_sq(step):
            copy.start()

    def row_copy(i):
        peer = lax.rem(mine + i, count)
        return pltpu.make_async_remote_copy(
            src_ref=rowbuf.at[mine], dst_ref=rowbuf.at[mine], send_sem=sq_send.at[i], recv_sem=sq_recv.at[i],
            device_id=(peer // ranks, lax.rem(peer, ranks)), device_id_type=MESH,
        )

    def begin(i, c):
        row_copy(i).start()
        return c

    def finish(i, c):
        row_copy(i).wait()
        return c

    lax.fori_loop(1, count, begin, 0)
    for step in range(1, ranks):
        for copy in send_sq(step):
            copy.wait()
    group_sum = sqbuf[0]
    for z in range(1, ranks):
        group_sum = group_sum + sqbuf[z]
    norm_out[...] = jnp.transpose(jnp.sqrt(group_sum))[0:4, :]
    lax.fori_loop(1, count, finish, 0)
    everything = lax.fori_loop(0, count, lambda i, c: c + rowbuf[i], jnp.zeros((1, LANES), jnp.float32))
    tot_out[...] = jnp.sqrt(everything[:, 0:4] / (scen * groups))


def put(mis, dual, lim, norm, tot, mis_out, dual_out, lim_out, norm_out, tot_out, sems):
    copies = [pltpu.make_async_copy(mis.at[q], mis_out.at[:, q], sems.at[q]) for q in range(2)]
    rest = ((dual, dual_out), (lim, lim_out), (norm, norm_out), (tot, tot_out))
    copies += [pltpu.make_async_copy(a, b, sems.at[2 + i]) for i, (a, b) in enumerate(rest)]
    for copy in copies:
        copy.start()
    for copy in copies:
        copy.wait()


def per_device(
    base_vm, base_va, delta_state, multipliers, net_inj, ang_grad, from_bus, to_bus,
    status, conduct, suscept, charging, rating, slack, zdual,
):
    groups, ranks = lax.axis_size("ctg"), lax.axis_size("br")
    count = groups * ranks
    scen, _, nb = delta_state.shape
    nl = from_bus.shape[0]
    per = scen // ranks
    buses, rows = nb * ranks, nl // LANES
    total = rows * ranks
    pad = -(-rows // SUB) * SUB
    piece = base_vm.shape[0]
    width, group, _, entries = packing(per)
    f32, i32 = jnp.float32, jnp.int32
    vmem = pl.BlockSpec(memory_space=pltpu.VMEM)
    hbm = pl.BlockSpec(memory_space=pl.ANY)
    sem = pltpu.SemaphoreType.DMA
    kinds = 8 + 2 * per
    shapes = (
        jax.ShapeDtypeStruct((2, scen, nb), f32),
        jax.ShapeDtypeStruct((scen, nb), f32),
        jax.ShapeDtypeStruct((scen, nl), f32),
        jax.ShapeDtypeStruct((4, scen), f32),
        jax.ShapeDtypeStruct((1, 4), f32),
    )

    def lined(x):
        return x.reshape(rows, LANES)

    made = pl.pallas_call(
        functools.partial(body, groups, ranks),
        out_shape=shapes,
        in_specs=[hbm] * 16,
        out_specs=(vmem,) * 5,
        scratch_shapes=[
            pltpu.VMEM((2, 1, piece), f32),
            pltpu.VMEM((groups, 2, 1, piece), f32),
            pltpu.VMEM((2, scen, nb), f32),
            pltpu.VMEM((SUB, buses), f32),
            pltpu.VMEM((2, total, LANES), i32),
            pltpu.VMEM((3, total, LANES), f32),
            pltpu.VMEM((per, total, LANES), i32),
            pltpu.VMEM((2, total * SUB, LANES), f32),
            pltpu.VMEM((2, entries * SUB, LANES), f32),
            pltpu.VMEM((buses // SPAN * width, SPAN), f32),
            pltpu.VMEM((ranks, 3, per, nb), f32),
            pltpu.VMEM((3, scen, nb), f32),
            pltpu.VMEM((per, total, LANES), f32),
            pltpu.VMEM((scen * pad, LANES), f32),
            pltpu.VMEM((scen, LANES), f32),
            pltpu.VMEM((ranks, scen, LANES), f32),
            pltpu.VMEM((count, 1, LANES), f32),
            pltpu.VMEM((2, scen, nb), f32),
            pltpu.VMEM((scen, nb), f32),
            pltpu.VMEM((scen, nl), i32),
            pltpu.VMEM((scen, nl), f32),
            pltpu.VMEM((scen, nl), f32),
            pltpu.VMEM((rows, LANES), f32),
            sem((20 + per,)),
            sem((kinds, ranks)),
            sem((kinds, ranks)),
            sem((groups,)),
            sem((groups,)),
            sem((count,)),
            sem((count,)),
        ],
        compiler_params=pltpu.CompilerParams(
            collective_id=0, has_side_effects=True, vmem_limit_bytes=67043328
        ),
    )(
        base_vm, base_va, delta_state, multipliers, net_inj, ang_grad, lined(from_bus), lined(to_bus),
        status.reshape(scen, rows, LANES).transpose(1, 0, 2),
        lined(conduct), lined(suscept), lined(charging), lined(rating), status, slack, zdual,
    )
    mis, dual, lim, norms, tot = pl.pallas_call(
        put,
        out_shape=(jax.ShapeDtypeStruct((scen, 2, nb), f32),) + shapes[1:],
        in_specs=[vmem] * 5,
        out_specs=(hbm,) * 5,
        scratch_shapes=[sem((6,))],
    )(*made)
    return (mis, dual, lim, norms.T, tot[0])


def solution(mesh):
    placed = (
        P(("ctg", "br")), P(("ctg", "br")),
        P("ctg", None, "br"), P("ctg", None, "br"), P("ctg", None, "br"), P("ctg", "br"),
        P("br"), P("br"), P("ctg", "br"), P("br"), P("br"), P("br"), P("br"),
        P("ctg", "br"), P("ctg", "br"),
    )
    return jax.shard_map(
        per_device,
        mesh=mesh,
        in_specs=placed,
        out_specs=(P("ctg", None, "br"), P("ctg", "br"), P("ctg", "br"), P("ctg", None), P()),
        check_vma=False,
    )
```

```python
import functools
import math

import jax
import jax.numpy as jnp
from jax import lax
from jax.experimental import pallas as pl
from jax.experimental.pallas import tpu as pltpu
from jax.sharding import PartitionSpec as P

LANES = 128
SPAN = 256
SUB = 8
PACK = 16
LOOP_GATHERS = 1
MESH = pl.DeviceIdType.MESH


def sin_cos(x):
    y = x * x
    sin_c = (1 / 6227020800, -1 / 39916800, 1 / 362880, -1 / 5040, 1 / 120, -1 / 6)
    cos_c = (-1 / 87178291200, 1 / 479001600, -1 / 3628800, 1 / 40320, -1 / 720, 1 / 24, -0.5)
    s = jnp.full_like(y, sin_c[0])
    for c in sin_c[1:]:
        s = s * y + c
    k = jnp.full_like(y, cos_c[0])
    for c in cos_c[1:]:
        k = k * y + c
    return x + x * y * s, 1.0 + y * k


def packing(per):
    width = 6 * per
    group = width * PACK // math.gcd(width, PACK)
    starts = [(SUB * h) % width for h in range(group // SUB)]
    return width, group, starts, max(starts) + SUB


def body(
    groups, ranks,
    bvm, bva, delta, mult, net_h, ang_h, frm, to, status_t, con, sus, cha, rat, status_h, slack_h, zdual_h,
    mis_out, dual_out, lim_out, norm_out, tot_out,
    bown, bslot, volts, table, split, ends, par, stat, picks, vals, acc, res, rbuf, flow, rflow,
    sqs, sqbuf, rowbuf, net, ang, status, slack, zdual, rate,
    local, send, recv, base_send, base_recv, sq_send, sq_recv,
):
    grp, me = lax.axis_index("ctg"), lax.axis_index("br")
    count = groups * ranks
    mine = grp * ranks + me
    scen, _, nb = delta.shape
    per = scen // ranks
    rows = frm.shape[0]
    total = rows * ranks
    pad = rflow.shape[0] // scen
    bf16 = jnp.bfloat16

    def cols_of(src):
        return pl.ds(pl.multiple_of(src * nb, LANES), nb)

    def rows_of(src):
        return pl.ds(src * rows, rows)

    def scen_of(src):
        return pl.ds(src * per, per)

    pairs = [(bvm, bown.at[0, 0]), (bva, bown.at[1, 0])]
    pairs += [(delta.at[:, q], volts.at[q]) for q in range(2)]
    pairs += [(frm, ends.at[0, rows_of(me)]), (to, ends.at[1, rows_of(me)])]
    pairs += [(p, par.at[i, rows_of(me)]) for i, p in enumerate((con, sus, cha))]
    early = len(pairs)
    pairs += [(delta.at[scen_of(me), q], table.at[pl.ds(q * per, per), cols_of(me)]) for q in range(2)]
    pairs += [(mult.at[scen_of(me), q], table.at[pl.ds((2 + q) * per, per), cols_of(me)]) for q in range(2)]
    pairs += [(status_t.at[:, me * per + s], stat.at[s, rows_of(me)]) for s in range(per)]
    middle = len(pairs)
    pairs += [(net_h.at[:, q], net.at[q]) for q in range(2)]
    pairs += [(ang_h, ang), (status_h, status), (slack_h, slack), (zdual_h, zdual), (rat, rate)]
    copies = [pltpu.make_async_copy(a, b, local.at[i]) for i, (a, b) in enumerate(pairs)]
    for copy in copies:
        copy.start()

    barrier = pltpu.get_barrier_semaphore()

    def greet(i, carry):
        peer = lax.rem(mine + i, count)
        pl.semaphore_signal(
            barrier, inc=1, device_id=(peer // ranks, lax.rem(peer, ranks)), device_id_type=MESH
        )
        return carry

    lax.fori_loop(1, count, greet, 0)
    acc[...] = jnp.zeros_like(acc)
    sqs[...] = jnp.zeros_like(sqs)
    for copy in copies[:early]:
        copy.wait()
    pl.semaphore_wait(barrier, count - 1)

    def toward(step):
        return lax.rem(me - step + ranks, ranks)

    def origin(step):
        return lax.rem(me + step, ranks)

    def remote(src, dst, kind, step):
        return pltpu.make_async_remote_copy(
            src_ref=src, dst_ref=dst, send_sem=send.at[kind, step], recv_sem=recv.at[kind, step],
            device_id=(grp, toward(step)), device_id_type=MESH,
        )

    def send_ends(step):
        return [remote(ends.at[:, rows_of(me)], ends.at[:, rows_of(me)], 0, step)]

    def send_mult(step):
        return [
            remote(mult.at[scen_of(toward(step)), q], table.at[pl.ds((2 + q) * per, per), cols_of(me)], 1 + q, step)
            for q in range(2)
        ]

    def send_volts(step):
        return [
            remote(volts.at[q, scen_of(toward(step))], table.at[pl.ds(q * per, per), cols_of(me)], 3 + q, step)
            for q in range(2)
        ]

    def send_par(step):
        return [remote(par.at[:, rows_of(me)], par.at[:, rows_of(me)], 5, step)] + [
            remote(status_t.at[:, toward(step) * per + s], stat.at[s, rows_of(me)], 6 + s, step)
            for s in range(per)
        ]

    def send_res(step):
        return [remote(res.at[toward(step)], rbuf.at[:, scen_of(me)], 6 + per, step)]

    def send_flow(step):
        return [
            remote(flow.at[s, rows_of(toward(step))], rflow.at[pl.ds((me * per + s) * pad, rows)], 7 + per + s, step)
            for s in range(per)
        ]

    def send_sq(step):
        return [remote(sqbuf.at[me], sqbuf.at[me], 7 + 2 * per, step)]

    for step in range(1, ranks):
        for copy in send_ends(step):
            copy.start()

    home = mine // groups

    def base_copy(i):
        return pltpu.make_async_remote_copy(
            src_ref=bown, dst_ref=bslot.at[mine - home * groups],
            send_sem=base_send.at[i], recv_sem=base_recv.at[mine - home * groups],
            device_id=(i, home), device_id_type=MESH,
        )

    def begin_base(i, c):
        @pl.when(jnp.logical_or(i != grp, home != me))
        def _():
            base_copy(i).start()
        return c

    lax.fori_loop(0, groups, begin_base, 0)

    @pl.when(home == me)
    def _():
        bslot[mine - me * groups] = bown[...]

    for step in range(1, ranks):
        for copy in send_mult(step):
            copy.start()

    def end_base(i, c):
        @pl.when(jnp.logical_or(i != grp, home != me))
        def _():
            base_copy(i).wait_send()

        @pl.when(me * groups + i != mine)
        def _():
            pltpu.make_async_remote_copy(
                src_ref=bown, dst_ref=bslot.at[i], send_sem=base_send.at[i], recv_sem=base_recv.at[i],
                device_id=(i, home), device_id_type=MESH,
            ).wait_recv()
        return c

    lax.fori_loop(0, groups, end_base, 0)
    for copy in copies[early:middle]:
        copy.wait()
    for q in range(2):
        base = jnp.concatenate([bslot[i, q] for i in range(groups)], axis=1)
        shift = 1.0 - q
        volts[q] = (volts[q] + base) - shift
        table[q * per : (q + 1) * per, cols_of(me)] = (table[q * per : (q + 1) * per, cols_of(me)] + base) - shift

    for step in range(1, ranks):
        for copy in send_volts(step):
            copy.start()
    for step in range(1, ranks):
        for copy in send_par(step):
            copy.start()

    tiles = nb // LANES

    def look(spot, src, found):
        low, tile = spot & (LANES - 1), (spot >> 7) - src * tiles
        for k in range(tiles):
            piece = jnp.take_along_axis(
                table[:, pl.ds(pl.multiple_of(src * nb + k * LANES, LANES), LANES)],
                low, axis=1, mode="promise_in_bounds",
            )
            found = jnp.where(tile == k, piece, found)
        return found

    def spot_of(end, r):
        return jnp.broadcast_to(ends[end, pl.ds(r, 1), :], (SUB, LANES))

    def slot_of(r):
        return pl.ds(pl.multiple_of(r * SUB, SUB), SUB)

    spans_here = nb // SPAN
    half = split.shape[1] // 2
    label = lax.broadcasted_iota(jnp.int32, (SPAN, LANES), 0).astype(bf16)

    def divide(src):
        for k in range(0, spans_here, 2):
            wide = [
                table[:, pl.ds(pl.multiple_of(src * nb + o * SPAN, LANES), SPAN)]
                for o in range(k, min(k + 2, spans_here))
            ]
            wide = jnp.concatenate((wide * 2)[:2], axis=0)
            head = wide.astype(bf16)
            split[src, k * SUB : k * SUB + PACK, :] = head
            split[src, half + k * SUB : half + k * SUB + PACK, :] = (wide - head.astype(jnp.float32)).astype(bf16)

    def hot_of(end, r):
        low = jnp.broadcast_to(ends[end, pl.ds(r, 1), :] & (SPAN - 1), (PACK, LANES)).astype(bf16)
        low = jnp.concatenate([low] * (SPAN // PACK), axis=0)
        return jnp.where(low == label, bf16(1), bf16(0))

    def multiply(r, srcs, found):
        hot = jnp.concatenate([hot_of(end, r) for end in range(2)], axis=1)
        left = jnp.concatenate([split[src] for src in srcs], axis=0)
        out = lax.dot_general(left, hot, (((1,), (0,)), ((), ())), preferred_element_type=jnp.float32)
        for end in range(2):
            at = slice(end * LANES, (end + 1) * LANES)
            span = spot_of(end, r) >> 8
            for n, src in enumerate(srcs):
                mark = span - src * spans_here
                for k in range(spans_here):
                    row = 2 * n * half + k * SUB
                    value = out[row : row + SUB, at] + out[half + row : half + row + SUB, at]
                    found[end] = jnp.where(mark == k, value, found[end])
        return found

    def lookup(r, found, dots, gathers):
        if dots:
            found = multiply(r, [origin(step) for step in dots], found)
        for step in gathers:
            for end in range(2):
                found[end] = look(spot_of(end, r), origin(step), found[end])
        for end in range(2):
            picks[end, slot_of(r), :] = found[end]

    unroll = 13 if rows % 13 == 0 else 1
    early_steps = max(1, ranks // 2)
    loop_steps = list(range(early_steps, ranks))
    loop_gathers = loop_steps[:LOOP_GATHERS]
    loop_dots = loop_steps[LOOP_GATHERS:]

    def scan_rows(step, block):
        def some(t, c):
            for o in range(unroll):
                r = block * rows + t * unroll + o
                if step == 0:
                    found = [jnp.zeros((SUB, LANES), jnp.float32)] * 2
                else:
                    found = [picks[end, slot_of(r), :] for end in range(2)]
                lookup(r, found, [step], [])
            return c

        lax.fori_loop(0, rows // unroll, some, 0)

    divide(me)
    for block in range(1, ranks):
        for copy in send_ends(block):
            copy.wait()
    for step in range(early_steps):
        if step > 0:
            for copy in send_mult(step) + send_volts(step):
                copy.wait()
            divide(origin(step))
        lax.fori_loop(0, ranks, lambda b, c, step=step: (scan_rows(step, b), c)[1], 0)
    for step in range(early_steps, ranks):
        for copy in send_mult(step) + send_volts(step):
            copy.wait()
    for step in loop_dots:
        divide(origin(step))

    for copy in copies[middle:]:
        copy.wait()

    chunks = total // SUB
    first = (me * rows + SUB - 1) // SUB
    ahead = first * SUB - me * rows

    def chunk_of(i):
        return lax.rem(first + i, chunks)

    def pick(i):
        at = chunk_of(i) * SUB
        for t in range(SUB):
            r = at + t
            lookup(r, [picks[end, slot_of(r), :] for end in range(2)], loop_dots, loop_gathers)

    width, group, starts, entries = packing(per)
    spans = table.shape[1] // SPAN
    tps = group // width
    parts = group // PACK
    iota16 = lax.broadcasted_iota(jnp.int32, (PACK, LANES), 0)
    moved = [((iota16 + PACK * p) // width).astype(bf16) for p in range(parts)]

    def process(i):
        at = pl.multiple_of(chunk_of(i) * SUB, SUB)
        here = pl.ds(at, SUB)

        def quantity(end, q, s):
            return picks[end, pl.ds(at * SUB + q * per + s, SUB, stride=SUB), :]

        seen = [[[quantity(end, q, s) for s in range(per)] for q in range(4)] for end in range(2)]
        pick(jnp.minimum(i + 1, chunks - 1))
        g, b, h = par[0, here, :], par[1, here, :], par[2, here, :]
        bh = -(b + h)
        for s in range(per):
            live = stat[s, here, :].astype(jnp.float32)
            vf, vt = 1.0 + seen[0][0][s], 1.0 + seen[1][0][s]
            sn, cs = sin_cos(seen[0][1][s] - seen[1][1][s])
            u = vf * vt
            gc_bs, gc_mbs = g * cs + b * sn, g * cs - b * sn
            gs_bc, gs_mbc = g * sn + b * cs, g * sn - b * cs
            pf = live * (g * vf * vf - u * gc_bs)
            qf = live * (bh * vf * vf - u * gs_mbc)
            pt = live * (g * vt * vt - u * gc_mbs)
            qt = live * (bh * vt * vt + u * gs_bc)
            fd = live * u * (
                seen[0][2][s] * gs_mbc - seen[0][3][s] * gc_bs
                + seen[1][2][s] * gs_bc + seen[1][3][s] * gc_mbs
            )
            flow[s, here, :] = pf * pf + qf * qf
            for end, terms in ((0, (pf, qf, fd)), (1, (pt, qt, -fd))):
                for q, term in enumerate(terms):
                    head = term.astype(bf16).astype(jnp.float32)
                    tail = term - head
                    for v, x in ((q * per + s, head), ((3 + q) * per + s, tail)):
                        for e in range(v, entries, width):
                            vals[end, e * SUB : (e + 1) * SUB, :] = x
        sums = None
        for end in range(2):
            for pair in range(SUB // 2):
                lefts, hots = [], []
                for t in (2 * pair, 2 * pair + 1):
                    spot = jnp.broadcast_to(ends[end, pl.ds(at + t, 1), :], (PACK, LANES))
                    high = (spot >> 8).astype(bf16)
                    hots.append(hot_of(end, at + t))
                    near = {
                        s0: vals[end, pl.ds(s0 * SUB + t, SUB, stride=SUB), :] for s0 in set(starts)
                    }
                    tile = [
                        jnp.concatenate([near[starts[2 * p]], near[starts[2 * p + 1]]], axis=0).astype(bf16)
                        for p in range(parts)
                    ]
                    level = [high - moved[p] for p in range(parts)]
                    lefts.append(jnp.concatenate([
                        jnp.where(level[p] == bf16(j * tps), tile[p], bf16(0))
                        for j in range(spans // tps) for p in range(parts)
                    ], axis=0))
                term = lax.dot_general(
                    jnp.concatenate(lefts, axis=1), jnp.concatenate(hots, axis=1),
                    (((1,), (1,)), ((), ())), preferred_element_type=jnp.float32,
                )
                sums = term if sums is None else sums + term
        acc[...] += sums

    pick(0)

    def advance(i, c):
        done = ahead + i * SUB

        for step in range(1, ranks):
            @pl.when(jnp.logical_and(done + SUB > step * rows, jnp.logical_or(done <= step * rows, i == 0)))
            def _(step=step):
                for copy in send_par(step):
                    copy.wait()

        process(i)

        for step in range(1, ranks):
            @pl.when(jnp.logical_and(done + SUB >= (step + 1) * rows, done < (step + 1) * rows))
            def _(step=step):
                for copy in send_flow(ranks - step):
                    copy.start()
        return c

    lax.fori_loop(0, chunks, advance, 0)

    quarter = nb // SPAN
    for dest in range(ranks):
        for k in range(dest * quarter, (dest + 1) * quarter):
            row = (k // tps) * group + (k % tps) * width
            both = acc[row : row + 3 * per, :] + acc[row + 3 * per : row + width, :]
            for q in range(3):
                at = (k - dest * quarter) * SPAN
                res[dest, q, :, at : at + SPAN] = both[q * per : (q + 1) * per, :]

        @pl.when(dest == me)
        def _(dest=dest):
            for q in range(3):
                rbuf[q, dest * per : (dest + 1) * per, :] = res[dest, q]

        for step in range(1, ranks):
            @pl.when(dest == toward(step))
            def _(step=step):
                for copy in send_res(step):
                    copy.start()

    for dest in range(ranks):
        @pl.when(dest == me)
        def _(dest=dest):
            for s in range(per):
                at = (dest * per + s) * pad
                rflow[at : at + rows, :] = flow[s, dest * rows : (dest + 1) * rows, :]

    live_own = status[...].astype(jnp.float32)
    comp = live_own * (zdual[...] * slack[...] - 0.01)
    sqs[:, 3:4] = jnp.sum(comp * comp, axis=1, keepdims=True)
    for step in range(1, ranks):
        for copy in send_flow(step):
            copy.wait()
    power = jnp.zeros((scen, LANES), jnp.float32)
    for r in range(rows):
        at = slice(r * LANES, (r + 1) * LANES)
        limit = rate[r : r + 1, :]
        lim = status[:, at].astype(jnp.float32) * (
            rflow[pl.ds(r, scen, stride=pad), :] + slack[:, at] - limit * limit
        )
        lim_out[:, at] = lim
        power = power + lim * lim
    sqs[:, 2:3] = jnp.sum(power, axis=1, keepdims=True)

    for step in range(1, ranks):
        for copy in send_res(step):
            copy.wait()
    power = None
    for q in range(2):
        row = rbuf[q] - net[q]
        mis_out[q] = row
        power = row * row if power is None else power + row * row
    sqs[:, 0:1] = jnp.sum(power, axis=1, keepdims=True)
    dual = rbuf[2] + ang[...]
    dual_out[...] = dual
    sqs[:, 1:2] = jnp.sum(dual * dual, axis=1, keepdims=True)

    sqbuf[me] = sqs[...]
    rowbuf[mine] = jnp.sum(sqs[...], axis=0, keepdims=True)
    for step in range(1, ranks):
        for copy in send_sq(step):
            copy.start()

    def row_copy(i):
        peer = lax.rem(mine + i, count)
        return pltpu.make_async_remote_copy(
            src_ref=rowbuf.at[mine], dst_ref=rowbuf.at[mine], send_sem=sq_send.at[i], recv_sem=sq_recv.at[i],
            device_id=(peer // ranks, lax.rem(peer, ranks)), device_id_type=MESH,
        )

    def begin(i, c):
        row_copy(i).start()
        return c

    def finish(i, c):
        row_copy(i).wait()
        return c

    lax.fori_loop(1, count, begin, 0)
    for step in range(1, ranks):
        for copy in send_sq(step):
            copy.wait()
    group_sum = sqbuf[0]
    for z in range(1, ranks):
        group_sum = group_sum + sqbuf[z]
    norm_out[...] = jnp.transpose(jnp.sqrt(group_sum))[0:4, :]
    lax.fori_loop(1, count, finish, 0)
    everything = lax.fori_loop(0, count, lambda i, c: c + rowbuf[i], jnp.zeros((1, LANES), jnp.float32))
    tot_out[...] = jnp.sqrt(everything[:, 0:4] / (scen * groups))


def put(mis, dual, lim, norm, tot, mis_out, dual_out, lim_out, norm_out, tot_out, sems):
    copies = [pltpu.make_async_copy(mis.at[q], mis_out.at[:, q], sems.at[q]) for q in range(2)]
    rest = ((dual, dual_out), (lim, lim_out), (norm, norm_out), (tot, tot_out))
    copies += [pltpu.make_async_copy(a, b, sems.at[2 + i]) for i, (a, b) in enumerate(rest)]
    for copy in copies:
        copy.start()
    for copy in copies:
        copy.wait()


def per_device(
    base_vm, base_va, delta_state, multipliers, net_inj, ang_grad, from_bus, to_bus,
    status, conduct, suscept, charging, rating, slack, zdual,
):
    groups, ranks = lax.axis_size("ctg"), lax.axis_size("br")
    count = groups * ranks
    scen, _, nb = delta_state.shape
    nl = from_bus.shape[0]
    per = scen // ranks
    buses, rows = nb * ranks, nl // LANES
    total = rows * ranks
    pad = -(-rows // SUB) * SUB
    piece = base_vm.shape[0]
    tall = -(-nb // SPAN // 2) * PACK
    width, group, _, entries = packing(per)
    f32, i32 = jnp.float32, jnp.int32
    vmem = pl.BlockSpec(memory_space=pltpu.VMEM)
    hbm = pl.BlockSpec(memory_space=pl.ANY)
    sem = pltpu.SemaphoreType.DMA
    kinds = 8 + 2 * per
    shapes = (
        jax.ShapeDtypeStruct((2, scen, nb), f32),
        jax.ShapeDtypeStruct((scen, nb), f32),
        jax.ShapeDtypeStruct((scen, nl), f32),
        jax.ShapeDtypeStruct((4, scen), f32),
        jax.ShapeDtypeStruct((1, 4), f32),
    )

    def lined(x):
        return x.reshape(rows, LANES)

    made = pl.pallas_call(
        functools.partial(body, groups, ranks),
        out_shape=shapes,
        in_specs=[hbm] * 16,
        out_specs=(vmem,) * 5,
        scratch_shapes=[
            pltpu.VMEM((2, 1, piece), f32),
            pltpu.VMEM((groups, 2, 1, piece), f32),
            pltpu.VMEM((2, scen, nb), f32),
            pltpu.VMEM((SUB, buses), f32),
            pltpu.VMEM((ranks, 2 * tall, SPAN), jnp.bfloat16),
            pltpu.VMEM((2, total, LANES), i32),
            pltpu.VMEM((3, total, LANES), f32),
            pltpu.VMEM((per, total, LANES), i32),
            pltpu.VMEM((2, total * SUB, LANES), f32),
            pltpu.VMEM((2, entries * SUB, LANES), f32),
            pltpu.VMEM((buses // SPAN * width, SPAN), f32),
            pltpu.VMEM((ranks, 3, per, nb), f32),
            pltpu.VMEM((3, scen, nb), f32),
            pltpu.VMEM((per, total, LANES), f32),
            pltpu.VMEM((scen * pad, LANES), f32),
            pltpu.VMEM((scen, LANES), f32),
            pltpu.VMEM((ranks, scen, LANES), f32),
            pltpu.VMEM((count, 1, LANES), f32),
            pltpu.VMEM((2, scen, nb), f32),
            pltpu.VMEM((scen, nb), f32),
            pltpu.VMEM((scen, nl), i32),
            pltpu.VMEM((scen, nl), f32),
            pltpu.VMEM((scen, nl), f32),
            pltpu.VMEM((rows, LANES), f32),
            sem((20 + per,)),
            sem((kinds, ranks)),
            sem((kinds, ranks)),
            sem((groups,)),
            sem((groups,)),
            sem((count,)),
            sem((count,)),
        ],
        compiler_params=pltpu.CompilerParams(
            collective_id=0, has_side_effects=True, vmem_limit_bytes=67043328
        ),
    )(
        base_vm, base_va, delta_state, multipliers, net_inj, ang_grad, lined(from_bus), lined(to_bus),
        status.reshape(scen, rows, LANES).transpose(1, 0, 2),
        lined(conduct), lined(suscept), lined(charging), lined(rating), status, slack, zdual,
    )
    mis, dual, lim, norms, tot = pl.pallas_call(
        put,
        out_shape=(jax.ShapeDtypeStruct((scen, 2, nb), f32),) + shapes[1:],
        in_specs=[vmem] * 5,
        out_specs=(hbm,) * 5,
        scratch_shapes=[sem((6,))],
    )(*made)
    return (mis, dual, lim, norms.T, tot[0])


def solution(mesh):
    placed = (
        P(("ctg", "br")), P(("ctg", "br")),
        P("ctg", None, "br"), P("ctg", None, "br"), P("ctg", None, "br"), P("ctg", "br"),
        P("br"), P("br"), P("ctg", "br"), P("br"), P("br"), P("br"), P("br"),
        P("ctg", "br"), P("ctg", "br"),
    )
    return jax.shard_map(
        per_device,
        mesh=mesh,
        in_specs=placed,
        out_specs=(P("ctg", None, "br"), P("ctg", "br"), P("ctg", "br"), P("ctg", None), P()),
        check_vma=False,
    )
```

```python
import functools
import math

import jax
import jax.numpy as jnp
from jax import lax
from jax.experimental import pallas as pl
from jax.experimental.pallas import tpu as pltpu
from jax.sharding import PartitionSpec as P

LANES = 128
SPAN = 256
SUB = 8
PACK = 16
LOOP_GATHERS = 0
LAG = 3
LEAD = 4
MESH = pl.DeviceIdType.MESH


def sin_cos(x):
    y = x * x
    sin_c = (1 / 6227020800, -1 / 39916800, 1 / 362880, -1 / 5040, 1 / 120, -1 / 6)
    cos_c = (-1 / 87178291200, 1 / 479001600, -1 / 3628800, 1 / 40320, -1 / 720, 1 / 24, -0.5)
    s = jnp.full_like(y, sin_c[0])
    for c in sin_c[1:]:
        s = s * y + c
    k = jnp.full_like(y, cos_c[0])
    for c in cos_c[1:]:
        k = k * y + c
    return x + x * y * s, 1.0 + y * k


def packing(per):
    width = 6 * per
    group = width * PACK // math.gcd(width, PACK)
    starts = [(SUB * h) % width for h in range(group // SUB)]
    return width, group, starts, max(starts) + SUB


def body(
    groups, ranks,
    bvm, bva, delta, mult, net_h, ang_h, frm, to, status_t, con, sus, cha, rat, status_h, slack_h, zdual_h,
    mis_hbm, dual_hbm, lim_hbm, norm_out, tot_out,
    mis_out, dual_out, lim_out, out_sems,
    bown, bslot, volts, table, split, ends, par, stat, picks, vals, acc, res, rbuf, flow, rflow,
    sqs, sqbuf, rowbuf, net, ang, status, slack, zdual, rate,
    local, send, recv, base_send, base_recv, sq_send, sq_recv,
    totals, found_at,
):
    grp, me = lax.axis_index("ctg"), lax.axis_index("br")
    count = groups * ranks
    mine = grp * ranks + me
    scen, _, nb = delta.shape
    per = scen // ranks
    rows = frm.shape[0]
    total = rows * ranks
    pad = rflow.shape[0] // scen
    bf16 = jnp.bfloat16

    def cols_of(src):
        return pl.ds(pl.multiple_of(src * nb, LANES), nb)

    def rows_of(src):
        return pl.ds(src * rows, rows)

    def scen_of(src):
        return pl.ds(src * per, per)

    pairs = [(bvm, bown.at[0, 0]), (bva, bown.at[1, 0])]
    pairs += [(delta.at[:, q], volts.at[q]) for q in range(2)]
    pairs += [(frm, ends.at[0, rows_of(me)]), (to, ends.at[1, rows_of(me)])]
    pairs += [(p, par.at[i, rows_of(me)]) for i, p in enumerate((con, sus, cha))]
    early = len(pairs)
    pairs += [(delta.at[scen_of(me), q], table.at[pl.ds(q * per, per), cols_of(me)]) for q in range(2)]
    pairs += [(mult.at[scen_of(me), q], table.at[pl.ds((2 + q) * per, per), cols_of(me)]) for q in range(2)]
    pairs += [(status_t.at[:, me * per + s], stat.at[s, rows_of(me)]) for s in range(per)]
    middle = len(pairs)
    pairs += [(net_h.at[:, q], net.at[q]) for q in range(2)]
    pairs += [(ang_h, ang), (status_h, status), (slack_h, slack), (zdual_h, zdual), (rat, rate)]
    copies = [pltpu.make_async_copy(a, b, local.at[i]) for i, (a, b) in enumerate(pairs)]
    for copy in copies:
        copy.start()

    barrier = pltpu.get_barrier_semaphore()

    def greet(i, carry):
        peer = lax.rem(mine + i, count)
        pl.semaphore_signal(
            barrier, inc=1, device_id=(peer // ranks, lax.rem(peer, ranks)), device_id_type=MESH
        )
        return carry

    lax.fori_loop(1, count, greet, 0)
    for q in range(2):
        acc[...] = pltpu.matmul_pop(totals[q])
        for slot in found_at[q]:
            acc[0 : slot.shape[0], :] = pltpu.matmul_pop(slot)
    sqs[...] = jnp.zeros_like(sqs)
    for copy in copies[:early]:
        copy.wait()
    pl.semaphore_wait(barrier, count - 1)

    def toward(step):
        return lax.rem(me - step + ranks, ranks)

    def origin(step):
        return lax.rem(me + step, ranks)

    def remote(src, dst, kind, step):
        return pltpu.make_async_remote_copy(
            src_ref=src, dst_ref=dst, send_sem=send.at[kind, step], recv_sem=recv.at[kind, step],
            device_id=(grp, toward(step)), device_id_type=MESH,
        )

    def send_ends(step):
        return [remote(ends.at[:, rows_of(me)], ends.at[:, rows_of(me)], 0, step)]

    def send_mult(step):
        return [
            remote(mult.at[scen_of(toward(step)), q], table.at[pl.ds((2 + q) * per, per), cols_of(me)], 1 + q, step)
            for q in range(2)
        ]

    def send_volts(step):
        return [
            remote(volts.at[q, scen_of(toward(step))], table.at[pl.ds(q * per, per), cols_of(me)], 3 + q, step)
            for q in range(2)
        ]

    def send_par(step):
        return [remote(par.at[:, rows_of(me)], par.at[:, rows_of(me)], 5, step)] + [
            remote(status_t.at[:, toward(step) * per + s], stat.at[s, rows_of(me)], 6 + s, step)
            for s in range(per)
        ]

    def send_res(step):
        return [remote(res.at[toward(step)], rbuf.at[:, scen_of(me)], 6 + per, step)]

    def send_flow(step):
        return [
            remote(flow.at[s, rows_of(toward(step))], rflow.at[pl.ds((me * per + s) * pad, rows)], 7 + per + s, step)
            for s in range(per)
        ]

    def send_sq(step):
        return [remote(sqbuf.at[me], sqbuf.at[me], 7 + 2 * per, step)]

    home = mine // groups

    def base_copy(i):
        return pltpu.make_async_remote_copy(
            src_ref=bown, dst_ref=bslot.at[mine - home * groups],
            send_sem=base_send.at[i], recv_sem=base_recv.at[mine - home * groups],
            device_id=(i, home), device_id_type=MESH,
        )

    def begin_base(i, c):
        @pl.when(jnp.logical_or(i != grp, home != me))
        def _():
            base_copy(i).start()
        return c

    lax.fori_loop(0, groups, begin_base, 0)

    @pl.when(home == me)
    def _():
        bslot[mine - me * groups] = bown[...]

    for step in range(1, ranks):
        for copy in send_ends(step):
            copy.start()

    early_steps = max(1, ranks // 2)
    for step in range(1, early_steps + 1):
        for copy in send_mult(step):
            copy.start()

    def end_base(i, c):
        @pl.when(jnp.logical_or(i != grp, home != me))
        def _():
            base_copy(i).wait_send()

        @pl.when(me * groups + i != mine)
        def _():
            pltpu.make_async_remote_copy(
                src_ref=bown, dst_ref=bslot.at[i], send_sem=base_send.at[i], recv_sem=base_recv.at[i],
                device_id=(i, home), device_id_type=MESH,
            ).wait_recv()
        return c

    lax.fori_loop(0, groups, end_base, 0)
    for copy in copies[early:middle]:
        copy.wait()
    for q in range(2):
        base = jnp.concatenate([bslot[i, q] for i in range(groups)], axis=1)
        shift = 1.0 - q
        volts[q] = (volts[q] + base) - shift
        table[q * per : (q + 1) * per, cols_of(me)] = (table[q * per : (q + 1) * per, cols_of(me)] + base) - shift

    for step in range(1, ranks):
        for copy in (send_mult(step) if step > early_steps else []) + send_volts(step):
            copy.start()
    for step in range(1, ranks):
        for copy in send_par(step):
            copy.start()

    tiles = nb // LANES

    def look(spot, src, found):
        low, tile = spot & (LANES - 1), (spot >> 7) - src * tiles
        for k in range(tiles):
            piece = jnp.take_along_axis(
                table[:, pl.ds(pl.multiple_of(src * nb + k * LANES, LANES), LANES)],
                low, axis=1, mode="promise_in_bounds",
            )
            found = jnp.where(tile == k, piece, found)
        return found

    def spot_of(end, r):
        return jnp.broadcast_to(ends[end, pl.ds(r, 1), :], (SUB, LANES))

    def slot_of(r):
        return pl.ds(pl.multiple_of(r * SUB, SUB), SUB)

    spans_here = nb // SPAN
    half = split.shape[1] // 2
    label = lax.broadcasted_iota(jnp.int32, (SPAN, LANES), 0).astype(bf16)

    def divide(src):
        for k in range(0, spans_here, 2):
            wide = [
                table[:, pl.ds(pl.multiple_of(src * nb + o * SPAN, LANES), SPAN)]
                for o in range(k, min(k + 2, spans_here))
            ]
            wide = jnp.concatenate((wide * 2)[:2], axis=0)
            head = wide.astype(bf16)
            split[src, k * SUB : k * SUB + PACK, :] = head
            split[src, half + k * SUB : half + k * SUB + PACK, :] = (wide - head.astype(jnp.float32)).astype(bf16)

    def hot_of(r):
        made = []
        for end in range(2):
            low = jnp.broadcast_to(ends[end, pl.ds(r, 1), :] & (SPAN - 1), (PACK, LANES)).astype(bf16)
            low = jnp.concatenate([low] * (SPAN // PACK), axis=0)
            made.append(jnp.where(low == label, bf16(1), bf16(0)))
        return jnp.concatenate(made, axis=1)

    def multiply(r, unit, turn, steps):
        slots = found_at[unit]
        first = (turn * len(steps)) % (len(slots) // len(steps) * len(steps))
        pltpu.matmul_push_rhs(hot_of(r), staging_register=0, mxu_index=unit)
        for n, step in enumerate(steps):
            src = origin(step)
            pltpu.matmul_acc_lhs(slots[first + n], split[src, :half], load_staged_rhs=0 if n == 0 else None)
            pltpu.matmul_acc_lhs(slots[first + n], split[src, half:])
        return [slots[first + n] for n in range(len(steps))]

    def choose(r, taken, steps, found):
        for slot, step in zip(taken, steps):
            out = pltpu.matmul_pop(slot)
            for end in range(2):
                at = slice(end * LANES, (end + 1) * LANES)
                mark = (spot_of(end, r) >> 8) - origin(step) * spans_here
                for k in range(spans_here):
                    found[end] = jnp.where(mark == k, out[k * SUB : (k + 1) * SUB, at], found[end])

    def gather(r, steps, found):
        for step in steps:
            for end in range(2):
                found[end] = look(spot_of(end, r), origin(step), found[end])

    def keep(r, found):
        for end in range(2):
            picks[end, slot_of(r), :] = found[end]

    loop_steps = list(range(early_steps, ranks))
    loop_gathers = loop_steps[:LOOP_GATHERS]
    loop_dots = loop_steps[LOOP_GATHERS:]

    def scan_rows(step, block):
        waiting = []

        def settle():
            r, taken = waiting.pop(0)
            if step == 0:
                found = [jnp.zeros((SUB, LANES), jnp.float32)] * 2
            else:
                found = [picks[end, slot_of(r), :] for end in range(2)]
            choose(r, taken, [step], found)
            keep(r, found)

        for o in range(rows):
            r = block * rows + o
            waiting.append((r, multiply(r, o % 2, o // 2, [step])))
            if len(waiting) > LAG:
                settle()
        while waiting:
            settle()

    divide(me)
    for block in range(1, ranks):
        for copy in send_ends(block):
            copy.wait()
    for step in range(early_steps):
        if step > 0:
            for copy in send_mult(step) + send_volts(step):
                copy.wait()
            divide(origin(step))
        lax.fori_loop(0, ranks, lambda b, c, step=step: (scan_rows(step, b), c)[1], 0)
    for step in range(early_steps, ranks):
        for copy in send_mult(step) + send_volts(step):
            copy.wait()
    for step in loop_dots:
        divide(origin(step))

    for copy in copies[middle:]:
        copy.wait()

    chunks = total // SUB
    first = (me * rows + SUB - 1) // SUB
    ahead = first * SUB - me * rows

    def chunk_of(i):
        return lax.rem(first + i, chunks)

    width, group, starts, entries = packing(per)
    spans = table.shape[1] // SPAN
    tps = group // width
    parts = group // PACK
    iota16 = lax.broadcasted_iota(jnp.int32, (PACK, LANES), 0)
    moved = [((iota16 + PACK * p) // width).astype(bf16) for p in range(parts)]

    def process(i):
        at = pl.multiple_of(chunk_of(i) * SUB, SUB)
        here = pl.ds(at, SUB)

        def quantity(end, q, s):
            return picks[end, pl.ds(at * SUB + q * per + s, SUB, stride=SUB), :]

        seen = [[[quantity(end, q, s) for s in range(per)] for q in range(4)] for end in range(2)]
        g, b, h = par[0, here, :], par[1, here, :], par[2, here, :]
        bh = -(b + h)
        for s in range(per):
            live = stat[s, here, :].astype(jnp.float32)
            vf, vt = 1.0 + seen[0][0][s], 1.0 + seen[1][0][s]
            sn, cs = sin_cos(seen[0][1][s] - seen[1][1][s])
            u = vf * vt
            gc_bs, gc_mbs = g * cs + b * sn, g * cs - b * sn
            gs_bc, gs_mbc = g * sn + b * cs, g * sn - b * cs
            pf = live * (g * vf * vf - u * gc_bs)
            qf = live * (bh * vf * vf - u * gs_mbc)
            pt = live * (g * vt * vt - u * gc_mbs)
            qt = live * (bh * vt * vt + u * gs_bc)
            fd = live * u * (
                seen[0][2][s] * gs_mbc - seen[0][3][s] * gc_bs
                + seen[1][2][s] * gs_bc + seen[1][3][s] * gc_mbs
            )
            flow[s, here, :] = pf * pf + qf * qf
            for end, terms in ((0, (pf, qf, fd)), (1, (pt, qt, -fd))):
                for q, term in enumerate(terms):
                    head = term.astype(bf16).astype(jnp.float32)
                    tail = term - head
                    for v, x in ((q * per + s, head), ((3 + q) * per + s, tail)):
                        for e in range(v, entries, width):
                            vals[end, e * SUB : (e + 1) * SUB, :] = x
        def left_of(t):
            lefts = []
            for end in range(2):
                spot = jnp.broadcast_to(ends[end, pl.ds(at + t, 1), :], (PACK, LANES))
                high = (spot >> 8).astype(bf16)
                near = {s0: vals[end, pl.ds(s0 * SUB + t, SUB, stride=SUB), :] for s0 in set(starts)}
                tile = [
                    jnp.concatenate([near[starts[2 * p]], near[starts[2 * p + 1]]], axis=0).astype(bf16)
                    for p in range(parts)
                ]
                level = [high - moved[p] for p in range(parts)]
                lefts.append(jnp.concatenate([
                    jnp.where(level[p] == bf16(j * tps), tile[p], bf16(0))
                    for j in range(spans // tps) for p in range(parts)
                ], axis=0))
            return jnp.concatenate(lefts, axis=1)

        def add(t):
            unit = t % 2
            pltpu.matmul_push_rhs(hot_of(at + t), staging_register=1, mxu_index=unit, transpose=True)
            pltpu.matmul_acc_lhs(totals[unit], left_of(t), load_staged_rhs=1)

        seek(i + 1, add)

    def seek(i, add):
        at = chunk_of(jnp.minimum(i, chunks - 1)) * SUB
        waiting = []

        def settle():
            r, taken = waiting.pop(0)
            found = [picks[end, slot_of(r), :] for end in range(2)]
            choose(r, taken, loop_dots, found)
            gather(r, loop_gathers, found)
            keep(r, found)

        for t in range(SUB):
            waiting.append((at + t, multiply(at + t, t % 2, t // 2, loop_dots) if loop_dots else []))
            if add is not None and t >= LEAD:
                add(t - LEAD)
            if len(waiting) > LAG:
                settle()
        while waiting:
            settle()
        if add is not None:
            for t in range(SUB - LEAD, SUB):
                add(t)

    seek(0, None)

    def advance(i, c):
        done = ahead + i * SUB

        for step in range(1, ranks):
            @pl.when(jnp.logical_and(done + SUB > step * rows, jnp.logical_or(done <= step * rows, i == 0)))
            def _(step=step):
                for copy in send_par(step):
                    copy.wait()

        process(i)

        for step in range(1, ranks):
            @pl.when(jnp.logical_and(done + SUB >= (step + 1) * rows, done < (step + 1) * rows))
            def _(step=step):
                for copy in send_flow(ranks - step):
                    copy.start()
        return c

    lax.fori_loop(0, chunks, advance, 0)

    acc[...] = pltpu.matmul_pop(totals[0]) + pltpu.matmul_pop(totals[1])
    quarter = nb // SPAN
    for dest in range(ranks):
        for k in range(dest * quarter, (dest + 1) * quarter):
            row = (k // tps) * group + (k % tps) * width
            both = acc[row : row + 3 * per, :] + acc[row + 3 * per : row + width, :]
            for q in range(3):
                at = (k - dest * quarter) * SPAN
                res[dest, q, :, at : at + SPAN] = both[q * per : (q + 1) * per, :]

        @pl.when(dest == me)
        def _(dest=dest):
            for q in range(3):
                rbuf[q, dest * per : (dest + 1) * per, :] = res[dest, q]

        for step in range(1, ranks):
            @pl.when(dest == toward(step))
            def _(step=step):
                for copy in send_res(step):
                    copy.start()

    for dest in range(ranks):
        @pl.when(dest == me)
        def _(dest=dest):
            for s in range(per):
                at = (dest * per + s) * pad
                rflow[at : at + rows, :] = flow[s, dest * rows : (dest + 1) * rows, :]

    live_own = status[...].astype(jnp.float32)
    comp = live_own * (zdual[...] * slack[...] - 0.01)
    sqs[:, 3:4] = jnp.sum(comp * comp, axis=1, keepdims=True)
    for step in range(1, ranks):
        for copy in send_flow(step):
            copy.wait()
    power = jnp.zeros((scen, LANES), jnp.float32)
    for r in range(rows):
        at = slice(r * LANES, (r + 1) * LANES)
        limit = rate[r : r + 1, :]
        lim = status[:, at].astype(jnp.float32) * (
            rflow[pl.ds(r, scen, stride=pad), :] + slack[:, at] - limit * limit
        )
        lim_out[:, at] = lim
        power = power + lim * lim
    sqs[:, 2:3] = jnp.sum(power, axis=1, keepdims=True)

    for step in range(1, ranks):
        for copy in send_res(step):
            copy.wait()
    power = None
    for q in range(2):
        row = rbuf[q] - net[q]
        mis_out[q] = row
        power = row * row if power is None else power + row * row
    sqs[:, 0:1] = jnp.sum(power, axis=1, keepdims=True)
    dual = rbuf[2] + ang[...]
    dual_out[...] = dual
    sqs[:, 1:2] = jnp.sum(dual * dual, axis=1, keepdims=True)
    written = [
        pltpu.make_async_copy(a, b, out_sems.at[i])
        for i, (a, b) in enumerate(((mis_out, mis_hbm), (dual_out, dual_hbm), (lim_out, lim_hbm)))
    ]

    def row_copy(i):
        peer = lax.rem(mine + i, count)
        return pltpu.make_async_remote_copy(
            src_ref=rowbuf.at[mine], dst_ref=rowbuf.at[mine], send_sem=sq_send, recv_sem=sq_recv,
            device_id=(peer // ranks, lax.rem(peer, ranks)), device_id_type=MESH,
        )

    def begin(i, c):
        row_copy(i).start()
        return c

    all_rows = pltpu.make_async_remote_copy(
        src_ref=rowbuf.at[pl.ds(0, count - 1)], dst_ref=rowbuf.at[pl.ds(0, count - 1)],
        send_sem=sq_send, recv_sem=sq_recv, device_id=(grp, toward(1)), device_id_type=MESH,
    )

    sqbuf[me] = sqs[...]
    rowbuf[mine] = jnp.sum(sqs[...], axis=0, keepdims=True)
    for step in range(1, ranks):
        for copy in send_sq(step):
            copy.start()
    lax.fori_loop(1, count, begin, 0)
    for copy in written:
        copy.start()
    for step in range(1, ranks):
        for copy in send_sq(step):
            copy.wait()
    group_sum = sqbuf[0]
    for z in range(1, ranks):
        group_sum = group_sum + sqbuf[z]

    norm_out[...] = jnp.transpose(jnp.sqrt(group_sum))[0:4, :]
    for copy in written:
        copy.wait()
    all_rows.wait()
    everything = jnp.sum(rowbuf[...], axis=0)
    tot_out[...] = jnp.sqrt(everything[:, 0:4] / (scen * groups))


def put(mis, dual, lim, norm, tot, mis_out, dual_out, lim_out, norm_out, tot_out, sems):
    copies = [pltpu.make_async_copy(mis.at[q], mis_out.at[:, q], sems.at[q]) for q in range(2)]
    rest = ((dual, dual_out), (lim, lim_out), (norm, norm_out), (tot, tot_out))
    copies += [pltpu.make_async_copy(a, b, sems.at[2 + i]) for i, (a, b) in enumerate(rest)]
    for copy in copies:
        copy.start()
    for copy in copies:
        copy.wait()


def per_device(
    base_vm, base_va, delta_state, multipliers, net_inj, ang_grad, from_bus, to_bus,
    status, conduct, suscept, charging, rating, slack, zdual,
):
    groups, ranks = lax.axis_size("ctg"), lax.axis_size("br")
    count = groups * ranks
    scen, _, nb = delta_state.shape
    nl = from_bus.shape[0]
    per = scen // ranks
    buses, rows = nb * ranks, nl // LANES
    total = rows * ranks
    pad = -(-rows // SUB) * SUB
    piece = base_vm.shape[0]
    tall = -(-nb // SPAN // 2) * PACK
    width, group, _, entries = packing(per)
    f32, i32 = jnp.float32, jnp.int32
    vmem = pl.BlockSpec(memory_space=pltpu.VMEM)
    hbm = pl.BlockSpec(memory_space=pl.ANY)
    sem = pltpu.SemaphoreType.DMA
    kinds = 8 + 2 * per
    shapes = (
        jax.ShapeDtypeStruct((2, scen, nb), f32),
        jax.ShapeDtypeStruct((scen, nb), f32),
        jax.ShapeDtypeStruct((scen, nl), f32),
        jax.ShapeDtypeStruct((4, scen), f32),
        jax.ShapeDtypeStruct((1, 4), f32),
    )

    def lined(x):
        return x.reshape(rows, LANES)

    def scoped(*refs):
        def inner(sums, slots):
            body(groups, ranks, *refs, sums, slots)

        pl.run_scoped(
            inner,
            [pltpu.ACC(q)((buses // SPAN * width, SPAN), f32) for q in range(2)],
            [[pltpu.ACC(q)((tall, SPAN), f32) for _ in range(4)] for q in range(2)],
        )

    made = pl.pallas_call(
        scoped,
        out_shape=shapes,
        in_specs=[hbm] * 16,
        out_specs=(hbm,) * 3 + (vmem,) * 2,
        scratch_shapes=[
            pltpu.VMEM((2, scen, nb), f32),
            pltpu.VMEM((scen, nb), f32),
            pltpu.VMEM((scen, nl), f32),
            sem((3,)),
            pltpu.VMEM((2, 1, piece), f32),
            pltpu.VMEM((groups, 2, 1, piece), f32),
            pltpu.VMEM((2, scen, nb), f32),
            pltpu.VMEM((SUB, buses), f32),
            pltpu.VMEM((ranks, 2 * tall, SPAN), jnp.bfloat16),
            pltpu.VMEM((2, total, LANES), i32),
            pltpu.VMEM((3, total, LANES), f32),
            pltpu.VMEM((per, total, LANES), i32),
            pltpu.VMEM((2, total * SUB, LANES), f32),
            pltpu.VMEM((2, entries * SUB, LANES), f32),
            pltpu.VMEM((buses // SPAN * width, SPAN), f32),
            pltpu.VMEM((ranks, 3, per, nb), f32),
            pltpu.VMEM((3, scen, nb), f32),
            pltpu.VMEM((per, total, LANES), f32),
            pltpu.VMEM((scen * pad, LANES), f32),
            pltpu.VMEM((scen, LANES), f32),
            pltpu.VMEM((ranks, scen, LANES), f32),
            pltpu.VMEM((count, 1, LANES), f32),
            pltpu.VMEM((2, scen, nb), f32),
            pltpu.VMEM((scen, nb), f32),
            pltpu.VMEM((scen, nl), i32),
            pltpu.VMEM((scen, nl), f32),
            pltpu.VMEM((scen, nl), f32),
            pltpu.VMEM((rows, LANES), f32),
            sem((20 + per,)),
            sem((kinds, ranks)),
            sem((kinds, ranks)),
            sem((groups,)),
            sem((groups,)),
            sem,
            sem,
        ],
        compiler_params=pltpu.CompilerParams(
            collective_id=0, has_side_effects=True, vmem_limit_bytes=67043328
        ),
    )(
        base_vm, base_va, delta_state, multipliers, net_inj, ang_grad, lined(from_bus), lined(to_bus),
        status.reshape(scen, rows, LANES).transpose(1, 0, 2),
        lined(conduct), lined(suscept), lined(charging), lined(rating), status, slack, zdual,
    )
    mis, dual, lim, norms, tot = pl.pallas_call(
        put,
        out_shape=(jax.ShapeDtypeStruct((scen, 2, nb), f32),) + shapes[1:],
        in_specs=[vmem] * 5,
        out_specs=(hbm,) * 5,
        scratch_shapes=[sem((6,))],
    )(*made)
    return (mis, dual, lim, norms.T, tot[0])


def solution(mesh):
    placed = (
        P(("ctg", "br")), P(("ctg", "br")),
        P("ctg", None, "br"), P("ctg", None, "br"), P("ctg", None, "br"), P("ctg", "br"),
        P("br"), P("br"), P("ctg", "br"), P("br"), P("br"), P("br"), P("br"),
        P("ctg", "br"), P("ctg", "br"),
    )
    return jax.shard_map(
        per_device,
        mesh=mesh,
        in_specs=placed,
        out_specs=(P("ctg", None, "br"), P("ctg", "br"), P("ctg", "br"), P("ctg", None), P()),
        check_vma=False,
    )
```

```python
import functools
import math

import jax
import jax.numpy as jnp
from jax import lax
from jax.experimental import pallas as pl
from jax.experimental.pallas import tpu as pltpu
from jax.sharding import PartitionSpec as P

LANES = 128
SPAN = 256
SUB = 8
PACK = 16
LOOP_GATHERS = 0
LAG = 3
LEAD = 4
MESH = pl.DeviceIdType.MESH


def sin_cos(x):
    y = x * x
    sin_c = (1 / 6227020800, -1 / 39916800, 1 / 362880, -1 / 5040, 1 / 120, -1 / 6)
    cos_c = (-1 / 87178291200, 1 / 479001600, -1 / 3628800, 1 / 40320, -1 / 720, 1 / 24, -0.5)
    s = jnp.full_like(y, sin_c[0])
    for c in sin_c[1:]:
        s = s * y + c
    k = jnp.full_like(y, cos_c[0])
    for c in cos_c[1:]:
        k = k * y + c
    return x + x * y * s, 1.0 + y * k


def packing(per):
    width = 6 * per
    group = width * PACK // math.gcd(width, PACK)
    starts = [(SUB * h) % width for h in range(group // SUB)]
    return width, group, starts, max(starts) + SUB


def body(
    groups, ranks,
    bvm, bva, delta, mult, net_h, ang_h, frm, to, status_t, con, sus, cha, rat, status_h, slack_h, zdual_h,
    mis_hbm, dual_hbm, lim_hbm, norm_out, tot_out,
    mis_out, dual_out, lim_out, out_sems,
    bown, bslot, volts, table, split, ends, par, stat, picks, vals, acc, res, rbuf, flow, rflow,
    sqs, sqbuf, rowbuf, net, ang, status, slack, zdual, rate,
    local, send, recv, base_send, base_recv, sq_send, sq_recv,
    totals, found_at,
):
    grp, me = lax.axis_index("ctg"), lax.axis_index("br")
    count = groups * ranks
    mine = grp * ranks + me
    scen, _, nb = delta.shape
    per = scen // ranks
    rows = frm.shape[0]
    total = rows * ranks
    pad = rflow.shape[0] // scen
    bf16 = jnp.bfloat16

    def cols_of(src):
        return pl.ds(pl.multiple_of(src * nb, LANES), nb)

    def rows_of(src):
        return pl.ds(src * rows, rows)

    def scen_of(src):
        return pl.ds(src * per, per)

    pairs = [(bvm, bown.at[0, 0]), (bva, bown.at[1, 0])]
    pairs += [(delta.at[:, q], volts.at[q]) for q in range(2)]
    pairs += [(frm, ends.at[0, rows_of(me)]), (to, ends.at[1, rows_of(me)])]
    pairs += [(p, par.at[i, rows_of(me)]) for i, p in enumerate((con, sus, cha))]
    early = len(pairs)
    pairs += [(delta.at[scen_of(me), q], table.at[pl.ds(q * per, per), cols_of(me)]) for q in range(2)]
    pairs += [(mult.at[scen_of(me), q], table.at[pl.ds((2 + q) * per, per), cols_of(me)]) for q in range(2)]
    pairs += [(status_t.at[:, me * per + s], stat.at[s, rows_of(me)]) for s in range(per)]
    middle = len(pairs)
    pairs += [(net_h.at[:, q], net.at[q]) for q in range(2)]
    pairs += [(ang_h, ang), (status_h, status), (slack_h, slack), (zdual_h, zdual), (rat, rate)]
    copies = [pltpu.make_async_copy(a, b, local.at[i]) for i, (a, b) in enumerate(pairs)]
    for copy in copies:
        copy.start()

    barrier = pltpu.get_barrier_semaphore()

    def greet(i, carry):
        peer = lax.rem(mine + i, count)
        pl.semaphore_signal(
            barrier, inc=1, device_id=(peer // ranks, lax.rem(peer, ranks)), device_id_type=MESH
        )
        return carry

    lax.fori_loop(1, count, greet, 0)
    for q in range(2):
        acc[...] = pltpu.matmul_pop(totals[q])
        for slot in found_at[q]:
            acc[0 : slot.shape[0], :] = pltpu.matmul_pop(slot)
    sqs[...] = jnp.zeros_like(sqs)
    for copy in copies[:early]:
        copy.wait()
    pl.semaphore_wait(barrier, count - 1)

    def toward(step):
        return lax.rem(me - step + ranks, ranks)

    def origin(step):
        return lax.rem(me + step, ranks)

    def remote(src, dst, kind, step):
        return pltpu.make_async_remote_copy(
            src_ref=src, dst_ref=dst, send_sem=send.at[kind, step], recv_sem=recv.at[kind, step],
            device_id=(grp, toward(step)), device_id_type=MESH,
        )

    def send_ends(step):
        return [remote(ends.at[:, rows_of(me)], ends.at[:, rows_of(me)], 0, step)]

    def send_mult(step):
        return [
            remote(mult.at[scen_of(toward(step)), q], table.at[pl.ds((2 + q) * per, per), cols_of(me)], 1 + q, step)
            for q in range(2)
        ]

    def send_volts(step):
        return [
            remote(volts.at[q, scen_of(toward(step))], table.at[pl.ds(q * per, per), cols_of(me)], 3 + q, step)
            for q in range(2)
        ]

    def send_par(step):
        return [remote(par.at[:, rows_of(me)], par.at[:, rows_of(me)], 5, step)] + [
            remote(status_t.at[:, toward(step) * per + s], stat.at[s, rows_of(me)], 6 + s, step)
            for s in range(per)
        ]

    def send_res(step):
        return [remote(res.at[toward(step)], rbuf.at[:, scen_of(me)], 6 + per, step)]

    def send_flow(step):
        return [
            remote(flow.at[s, rows_of(toward(step))], rflow.at[pl.ds((me * per + s) * pad, rows)], 7 + per + s, step)
            for s in range(per)
        ]

    def send_sq(step):
        return [remote(sqbuf.at[me], sqbuf.at[me], 7 + 2 * per, step)]

    home = mine // groups

    def base_copy(i):
        return pltpu.make_async_remote_copy(
            src_ref=bown, dst_ref=bslot.at[mine - home * groups],
            send_sem=base_send.at[i], recv_sem=base_recv.at[mine - home * groups],
            device_id=(i, home), device_id_type=MESH,
        )

    def begin_base(i, c):
        @pl.when(jnp.logical_or(i != grp, home != me))
        def _():
            base_copy(i).start()
        return c

    lax.fori_loop(0, groups, begin_base, 0)

    @pl.when(home == me)
    def _():
        bslot[mine - me * groups] = bown[...]

    for step in range(1, ranks):
        for copy in send_ends(step):
            copy.start()

    early_steps = max(1, ranks // 2)
    for step in range(1, early_steps + 1):
        for copy in send_mult(step):
            copy.start()

    def end_base(i, c):
        @pl.when(jnp.logical_or(i != grp, home != me))
        def _():
            base_copy(i).wait_send()

        @pl.when(me * groups + i != mine)
        def _():
            pltpu.make_async_remote_copy(
                src_ref=bown, dst_ref=bslot.at[i], send_sem=base_send.at[i], recv_sem=base_recv.at[i],
                device_id=(i, home), device_id_type=MESH,
            ).wait_recv()
        return c

    lax.fori_loop(0, groups, end_base, 0)
    for copy in copies[early:middle]:
        copy.wait()
    for q in range(2):
        base = jnp.concatenate([bslot[i, q] for i in range(groups)], axis=1)
        shift = 1.0 - q
        volts[q] = (volts[q] + base) - shift
        table[q * per : (q + 1) * per, cols_of(me)] = (table[q * per : (q + 1) * per, cols_of(me)] + base) - shift

    for step in range(1, ranks):
        for copy in (send_mult(step) if step > early_steps else []) + send_volts(step):
            copy.start()
    for step in range(1, ranks):
        for copy in send_par(step):
            copy.start()

    tiles = nb // LANES

    def look(spot, src, found):
        low, tile = spot & (LANES - 1), (spot >> 7) - src * tiles
        for k in range(tiles):
            piece = jnp.take_along_axis(
                table[:, pl.ds(pl.multiple_of(src * nb + k * LANES, LANES), LANES)],
                low, axis=1, mode="promise_in_bounds",
            )
            found = jnp.where(tile == k, piece, found)
        return found

    def spot_of(end, r):
        return jnp.broadcast_to(ends[end, pl.ds(r, 1), :], (SUB, LANES))

    def slot_of(r):
        return pl.ds(pl.multiple_of(r * SUB, SUB), SUB)

    spans_here = nb // SPAN
    half = split.shape[1] // 2
    label = lax.broadcasted_iota(jnp.int32, (SPAN, LANES), 0).astype(bf16)

    def divide(src):
        for k in range(0, spans_here, 2):
            wide = [
                table[:, pl.ds(pl.multiple_of(src * nb + o * SPAN, LANES), SPAN)]
                for o in range(k, min(k + 2, spans_here))
            ]
            wide = jnp.concatenate((wide * 2)[:2], axis=0)
            head = wide.astype(bf16)
            split[src, k * SUB : k * SUB + PACK, :] = head
            split[src, half + k * SUB : half + k * SUB + PACK, :] = (wide - head.astype(jnp.float32)).astype(bf16)

    def hot_of(r):
        made = []
        for end in range(2):
            low = jnp.broadcast_to(ends[end, pl.ds(r, 1), :] & (SPAN - 1), (PACK, LANES)).astype(bf16)
            low = jnp.concatenate([low] * (SPAN // PACK), axis=0)
            made.append(jnp.where(low == label, bf16(1), bf16(0)))
        return jnp.concatenate(made, axis=1)

    def multiply(r, unit, turn, steps):
        slots = found_at[unit]
        first = (turn * len(steps)) % (len(slots) // len(steps) * len(steps))
        pltpu.matmul_push_rhs(hot_of(r), staging_register=0, mxu_index=unit)
        for n, step in enumerate(steps):
            src = origin(step)
            pltpu.matmul_acc_lhs(slots[first + n], split[src, :half], load_staged_rhs=0 if n == 0 else None)
            pltpu.matmul_acc_lhs(slots[first + n], split[src, half:])
        return [slots[first + n] for n in range(len(steps))]

    def choose(r, taken, steps, found):
        for slot, step in zip(taken, steps):
            out = pltpu.matmul_pop(slot)
            for end in range(2):
                at = slice(end * LANES, (end + 1) * LANES)
                mark = (spot_of(end, r) >> 8) - origin(step) * spans_here
                for k in range(spans_here):
                    found[end] = jnp.where(mark == k, out[k * SUB : (k + 1) * SUB, at], found[end])

    def gather(r, steps, found):
        for step in steps:
            for end in range(2):
                found[end] = look(spot_of(end, r), origin(step), found[end])

    def keep(r, found):
        for end in range(2):
            picks[end, slot_of(r), :] = found[end]

    loop_steps = list(range(early_steps, ranks))
    loop_gathers = loop_steps[:LOOP_GATHERS]
    loop_dots = loop_steps[LOOP_GATHERS:]

    def scan_rows(step, block):
        waiting = []

        def settle():
            r, taken = waiting.pop(0)
            if step == 0:
                found = [jnp.zeros((SUB, LANES), jnp.float32)] * 2
            else:
                found = [picks[end, slot_of(r), :] for end in range(2)]
            choose(r, taken, [step], found)
            keep(r, found)

        for o in range(rows):
            r = block * rows + o
            waiting.append((r, multiply(r, o % 2, o // 2, [step])))
            if len(waiting) > LAG:
                settle()
        while waiting:
            settle()

    divide(me)
    for step in range(early_steps):
        if step > 0:
            for copy in send_mult(step) + send_volts(step):
                copy.wait()
            divide(origin(step))
        start = 0
        if step == 0:
            start = 1
            scan_rows(0, me)
            for block in range(1, ranks):
                for copy in send_ends(block):
                    copy.wait()
        lax.fori_loop(start, ranks, lambda b, c, step=step: (scan_rows(step, origin(b)), c)[1], 0)
    for step in range(early_steps, ranks):
        for copy in send_mult(step) + send_volts(step):
            copy.wait()
    for step in loop_dots:
        divide(origin(step))

    for copy in copies[middle:]:
        copy.wait()

    chunks = total // SUB
    first = (me * rows + SUB - 1) // SUB
    ahead = first * SUB - me * rows

    def chunk_of(i):
        return lax.rem(first + i, chunks)

    width, group, starts, entries = packing(per)
    spans = table.shape[1] // SPAN
    tps = group // width
    parts = group // PACK
    iota16 = lax.broadcasted_iota(jnp.int32, (PACK, LANES), 0)
    moved = [((iota16 + PACK * p) // width).astype(bf16) for p in range(parts)]

    def process(i):
        at = pl.multiple_of(chunk_of(i) * SUB, SUB)
        here = pl.ds(at, SUB)

        def quantity(end, q, s):
            return picks[end, pl.ds(at * SUB + q * per + s, SUB, stride=SUB), :]

        seen = [[[quantity(end, q, s) for s in range(per)] for q in range(4)] for end in range(2)]
        g, b, h = par[0, here, :], par[1, here, :], par[2, here, :]
        bh = -(b + h)
        for s in range(per):
            live = stat[s, here, :].astype(jnp.float32)
            vf, vt = 1.0 + seen[0][0][s], 1.0 + seen[1][0][s]
            sn, cs = sin_cos(seen[0][1][s] - seen[1][1][s])
            u = vf * vt
            gc_bs, gc_mbs = g * cs + b * sn, g * cs - b * sn
            gs_bc, gs_mbc = g * sn + b * cs, g * sn - b * cs
            pf = live * (g * vf * vf - u * gc_bs)
            qf = live * (bh * vf * vf - u * gs_mbc)
            pt = live * (g * vt * vt - u * gc_mbs)
            qt = live * (bh * vt * vt + u * gs_bc)
            fd = live * u * (
                seen[0][2][s] * gs_mbc - seen[0][3][s] * gc_bs
                + seen[1][2][s] * gs_bc + seen[1][3][s] * gc_mbs
            )
            flow[s, here, :] = pf * pf + qf * qf
            for end, terms in ((0, (pf, qf, fd)), (1, (pt, qt, -fd))):
                for q, term in enumerate(terms):
                    head = term.astype(bf16).astype(jnp.float32)
                    tail = term - head
                    for v, x in ((q * per + s, head), ((3 + q) * per + s, tail)):
                        for e in range(v, entries, width):
                            vals[end, e * SUB : (e + 1) * SUB, :] = x
        def left_of(t):
            lefts = []
            for end in range(2):
                spot = jnp.broadcast_to(ends[end, pl.ds(at + t, 1), :], (PACK, LANES))
                high = (spot >> 8).astype(bf16)
                near = {s0: vals[end, pl.ds(s0 * SUB + t, SUB, stride=SUB), :] for s0 in set(starts)}
                tile = [
                    jnp.concatenate([near[starts[2 * p]], near[starts[2 * p + 1]]], axis=0).astype(bf16)
                    for p in range(parts)
                ]
                level = [high - moved[p] for p in range(parts)]
                lefts.append(jnp.concatenate([
                    jnp.where(level[p] == bf16(j * tps), tile[p], bf16(0))
                    for j in range(spans // tps) for p in range(parts)
                ], axis=0))
            return jnp.concatenate(lefts, axis=1)

        def add(t):
            unit = t % 2
            pltpu.matmul_push_rhs(hot_of(at + t), staging_register=1, mxu_index=unit, transpose=True)
            pltpu.matmul_acc_lhs(totals[unit], left_of(t), load_staged_rhs=1)

        seek(i + 1, add)

    def seek(i, add):
        at = chunk_of(jnp.minimum(i, chunks - 1)) * SUB
        waiting = []

        def settle():
            r, taken = waiting.pop(0)
            found = [picks[end, slot_of(r), :] for end in range(2)]
            choose(r, taken, loop_dots, found)
            gather(r, loop_gathers, found)
            keep(r, found)

        for t in range(SUB):
            waiting.append((at + t, multiply(at + t, t % 2, t // 2, loop_dots) if loop_dots else []))
            if add is not None and t >= LEAD:
                add(t - LEAD)
            if len(waiting) > LAG:
                settle()
        while waiting:
            settle()
        if add is not None:
            for t in range(SUB - LEAD, SUB):
                add(t)

    seek(0, None)

    def advance(i, c):
        done = ahead + i * SUB

        for step in range(1, ranks):
            @pl.when(jnp.logical_and(done + SUB > step * rows, jnp.logical_or(done <= step * rows, i == 0)))
            def _(step=step):
                for copy in send_par(step):
                    copy.wait()

        process(i)

        for step in range(1, ranks):
            @pl.when(jnp.logical_and(done + SUB >= (step + 1) * rows, done < (step + 1) * rows))
            def _(step=step):
                for copy in send_flow(ranks - step):
                    copy.start()
        return c

    lax.fori_loop(0, chunks, advance, 0)

    acc[...] = pltpu.matmul_pop(totals[0]) + pltpu.matmul_pop(totals[1])
    quarter = nb // SPAN
    for dest in [0, *range(ranks - 1, 0, -1)]:
        for k in range(dest * quarter, (dest + 1) * quarter):
            row = (k // tps) * group + (k % tps) * width
            both = acc[row : row + 3 * per, :] + acc[row + 3 * per : row + width, :]
            for q in range(3):
                at = (k - dest * quarter) * SPAN
                res[dest, q, :, at : at + SPAN] = both[q * per : (q + 1) * per, :]

        @pl.when(dest == me)
        def _(dest=dest):
            for q in range(3):
                rbuf[q, dest * per : (dest + 1) * per, :] = res[dest, q]

        for step in range(1, ranks):
            @pl.when(dest == toward(step))
            def _(step=step):
                for copy in send_res(step):
                    copy.start()

    for dest in range(ranks):
        @pl.when(dest == me)
        def _(dest=dest):
            for s in range(per):
                at = (dest * per + s) * pad
                rflow[at : at + rows, :] = flow[s, dest * rows : (dest + 1) * rows, :]

    live_own = status[...].astype(jnp.float32)
    comp = live_own * (zdual[...] * slack[...] - 0.01)
    sqs[:, 3:4] = jnp.sum(comp * comp, axis=1, keepdims=True)
    for step in range(1, ranks):
        for copy in send_flow(step):
            copy.wait()
    power = jnp.zeros((scen, LANES), jnp.float32)
    for r in range(rows):
        at = slice(r * LANES, (r + 1) * LANES)
        limit = rate[r : r + 1, :]
        lim = status[:, at].astype(jnp.float32) * (
            rflow[pl.ds(r, scen, stride=pad), :] + slack[:, at] - limit * limit
        )
        lim_out[:, at] = lim
        power = power + lim * lim
    sqs[:, 2:3] = jnp.sum(power, axis=1, keepdims=True)

    for step in range(1, ranks):
        for copy in send_res(step):
            copy.wait()
    power = None
    for q in range(2):
        row = rbuf[q] - net[q]
        mis_out[q] = row
        power = row * row if power is None else power + row * row
    sqs[:, 0:1] = jnp.sum(power, axis=1, keepdims=True)
    dual = rbuf[2] + ang[...]
    dual_out[...] = dual
    sqs[:, 1:2] = jnp.sum(dual * dual, axis=1, keepdims=True)
    written = [
        pltpu.make_async_copy(a, b, out_sems.at[i])
        for i, (a, b) in enumerate(((mis_out, mis_hbm), (dual_out, dual_hbm), (lim_out, lim_hbm)))
    ]

    def row_copy(i):
        peer = lax.rem(mine + i, count)
        return pltpu.make_async_remote_copy(
            src_ref=rowbuf.at[mine], dst_ref=rowbuf.at[mine], send_sem=sq_send, recv_sem=sq_recv,
            device_id=(peer // ranks, lax.rem(peer, ranks)), device_id_type=MESH,
        )

    def begin(i, c):
        row_copy(i).start()
        return c

    all_rows = pltpu.make_async_remote_copy(
        src_ref=rowbuf.at[pl.ds(0, count - 1)], dst_ref=rowbuf.at[pl.ds(0, count - 1)],
        send_sem=sq_send, recv_sem=sq_recv, device_id=(grp, toward(1)), device_id_type=MESH,
    )

    sqbuf[me] = sqs[...]
    rowbuf[mine] = jnp.sum(sqs[...], axis=0, keepdims=True)
    for step in range(1, ranks):
        for copy in send_sq(step):
            copy.start()
    lax.fori_loop(1, count, begin, 0)
    for copy in written:
        copy.start()
    for step in range(1, ranks):
        for copy in send_sq(step):
            copy.wait()
    group_sum = sqbuf[0]
    for z in range(1, ranks):
        group_sum = group_sum + sqbuf[z]

    norm_out[...] = jnp.transpose(jnp.sqrt(group_sum))[0:4, :]
    for copy in written:
        copy.wait()
    all_rows.wait()
    everything = jnp.sum(rowbuf[...], axis=0)
    tot_out[...] = jnp.sqrt(everything[:, 0:4] / (scen * groups))


def put(mis, dual, lim, norm, tot, mis_out, dual_out, lim_out, norm_out, tot_out, sems):
    copies = [pltpu.make_async_copy(mis.at[q], mis_out.at[:, q], sems.at[q]) for q in range(2)]
    rest = ((dual, dual_out), (lim, lim_out), (norm, norm_out), (tot, tot_out))
    copies += [pltpu.make_async_copy(a, b, sems.at[2 + i]) for i, (a, b) in enumerate(rest)]
    for copy in copies:
        copy.start()
    for copy in copies:
        copy.wait()


def per_device(
    base_vm, base_va, delta_state, multipliers, net_inj, ang_grad, from_bus, to_bus,
    status, conduct, suscept, charging, rating, slack, zdual,
):
    groups, ranks = lax.axis_size("ctg"), lax.axis_size("br")
    count = groups * ranks
    scen, _, nb = delta_state.shape
    nl = from_bus.shape[0]
    per = scen // ranks
    buses, rows = nb * ranks, nl // LANES
    total = rows * ranks
    pad = -(-rows // SUB) * SUB
    piece = base_vm.shape[0]
    tall = -(-nb // SPAN // 2) * PACK
    width, group, _, entries = packing(per)
    f32, i32 = jnp.float32, jnp.int32
    vmem = pl.BlockSpec(memory_space=pltpu.VMEM)
    hbm = pl.BlockSpec(memory_space=pl.ANY)
    sem = pltpu.SemaphoreType.DMA
    kinds = 8 + 2 * per
    shapes = (
        jax.ShapeDtypeStruct((2, scen, nb), f32),
        jax.ShapeDtypeStruct((scen, nb), f32),
        jax.ShapeDtypeStruct((scen, nl), f32),
        jax.ShapeDtypeStruct((4, scen), f32),
        jax.ShapeDtypeStruct((1, 4), f32),
    )

    def lined(x):
        return x.reshape(rows, LANES)

    def scoped(*refs):
        def inner(sums, slots):
            body(groups, ranks, *refs, sums, slots)

        pl.run_scoped(
            inner,
            [pltpu.ACC(q)((buses // SPAN * width, SPAN), f32) for q in range(2)],
            [[pltpu.ACC(q)((tall, SPAN), f32) for _ in range(4)] for q in range(2)],
        )

    made = pl.pallas_call(
        scoped,
        out_shape=shapes,
        in_specs=[hbm] * 16,
        out_specs=(hbm,) * 3 + (vmem,) * 2,
        scratch_shapes=[
            pltpu.VMEM((2, scen, nb), f32),
            pltpu.VMEM((scen, nb), f32),
            pltpu.VMEM((scen, nl), f32),
            sem((3,)),
            pltpu.VMEM((2, 1, piece), f32),
            pltpu.VMEM((groups, 2, 1, piece), f32),
            pltpu.VMEM((2, scen, nb), f32),
            pltpu.VMEM((SUB, buses), f32),
            pltpu.VMEM((ranks, 2 * tall, SPAN), jnp.bfloat16),
            pltpu.VMEM((2, total, LANES), i32),
            pltpu.VMEM((3, total, LANES), f32),
            pltpu.VMEM((per, total, LANES), i32),
            pltpu.VMEM((2, total * SUB, LANES), f32),
            pltpu.VMEM((2, entries * SUB, LANES), f32),
            pltpu.VMEM((buses // SPAN * width, SPAN), f32),
            pltpu.VMEM((ranks, 3, per, nb), f32),
            pltpu.VMEM((3, scen, nb), f32),
            pltpu.VMEM((per, total, LANES), f32),
            pltpu.VMEM((scen * pad, LANES), f32),
            pltpu.VMEM((scen, LANES), f32),
            pltpu.VMEM((ranks, scen, LANES), f32),
            pltpu.VMEM((count, 1, LANES), f32),
            pltpu.VMEM((2, scen, nb), f32),
            pltpu.VMEM((scen, nb), f32),
            pltpu.VMEM((scen, nl), i32),
            pltpu.VMEM((scen, nl), f32),
            pltpu.VMEM((scen, nl), f32),
            pltpu.VMEM((rows, LANES), f32),
            sem((20 + per,)),
            sem((kinds, ranks)),
            sem((kinds, ranks)),
            sem((groups,)),
            sem((groups,)),
            sem,
            sem,
        ],
        compiler_params=pltpu.CompilerParams(
            collective_id=0, has_side_effects=True, vmem_limit_bytes=67043328
        ),
    )(
        base_vm, base_va, delta_state, multipliers, net_inj, ang_grad, lined(from_bus), lined(to_bus),
        status.reshape(scen, rows, LANES).transpose(1, 0, 2),
        lined(conduct), lined(suscept), lined(charging), lined(rating), status, slack, zdual,
    )
    mis, dual, lim, norms, tot = pl.pallas_call(
        put,
        out_shape=(jax.ShapeDtypeStruct((scen, 2, nb), f32),) + shapes[1:],
        in_specs=[vmem] * 5,
        out_specs=(hbm,) * 5,
        scratch_shapes=[sem((6,))],
    )(*made)
    return (mis, dual, lim, norms.T, tot[0])


def solution(mesh):
    placed = (
        P(("ctg", "br")), P(("ctg", "br")),
        P("ctg", None, "br"), P("ctg", None, "br"), P("ctg", None, "br"), P("ctg", "br"),
        P("br"), P("br"), P("ctg", "br"), P("br"), P("br"), P("br"), P("br"),
        P("ctg", "br"), P("ctg", "br"),
    )
    return jax.shard_map(
        per_device,
        mesh=mesh,
        in_specs=placed,
        out_specs=(P("ctg", None, "br"), P("ctg", "br"), P("ctg", "br"), P("ctg", None), P()),
        check_vma=False,
    )
```
